32 devices in a mesh: wide: 8 (over z, x), group: 4 (over y, core).
Axes of the slice: x: 2, y: 2, z: 4, core: 2. Of those that a mesh axis runs over, the one named last changes fastest.
Arguments:
- feat4: bfloat16 [32, 24, 24, 256], P(('wide', 'group')), may hold values from -100 to 100
- feat5: bfloat16 [32, 12, 12, 256], P(('wide', 'group')), may hold values from -100 to 100
- feat6: bfloat16 [32, 6, 6, 256], P(('wide', 'group')), may hold values from -100 to 100
- feat7: bfloat16 [32, 3, 3, 256], P(('wide', 'group')), may hold values from -100 to 100
- out_grad4: bfloat16 [32, 24, 24, 256], P(('wide', 'group')), may hold values from -6 to 6
- out_grad5: bfloat16 [32, 12, 12, 256], P(('wide', 'group')), may hold values from -6 to 6
- out_grad6: bfloat16 [32, 6, 6, 256], P(('wide', 'group')), may hold values from -6 to 6
- out_grad7: bfloat16 [32, 3, 3, 256], P(('wide', 'group')), may hold values from -6 to 6
- conv_weight: bfloat16 [3, 3, 256, 256], replicated, may hold values from -0.125 to 0.125
- bn_gain: float32 [4, 256], replicated, may hold values from 0.25 to 1.75
- bn_shift: float32 [4, 256], replicated, may hold values from -0.5 to 0.5
- heights: int32 [32], P(('wide', 'group')), may hold values from 168 to 384
- widths: int32 [32], P(('wide', 'group')), may hold values from 168 to 384
Outputs:
- out4: bfloat16 [32, 24, 24, 256], P(('wide', 'group'))
- out5: bfloat16 [32, 12, 12, 256], P(('wide', 'group'))
- out6: bfloat16 [32, 6, 6, 256], P(('wide', 'group'))
- out7: bfloat16 [32, 3, 3, 256], P(('wide', 'group'))
- d_feat4: bfloat16 [32, 24, 24, 256], P(('wide', 'group'))
- d_feat5: bfloat16 [32, 12, 12, 256], P(('wide', 'group'))
- d_feat6: bfloat16 [32, 6, 6, 256], P(('wide', 'group'))
- d_feat7: bfloat16 [32, 3, 3, 256], P(('wide', 'group'))
- d_weight: float32 [3, 3, 256, 256], replicated
- d_gain: float32 [4, 256], replicated
- d_shift: float32 [4, 256], replicated
The draws below stay inside these ranges and needn't reach their ends.
Inputs may be any that keep to these rules, and one draw needn't show every extreme that they name: `heights`: pixel height of the valid part of each image. `widths`: pixel width of the valid part of each image.
All inputs are finite; a program needn't handle non-finite values.
Results may differ from the reference program's by a relative error of at most 0.0049.
Values sent between devices are 32-bit elements; how exact they have to be, the bound alone decides.
No kernel may reach another device: no remote copies, remote signals or barrier semaphores. Data moves between devices by JAX's collectives and lax.ppermute only.
A program may use at most 64 MiB of HBM per device.

```python
from functools import partial
import jax
import jax.numpy as jnp
from jax import lax

CH = 256
SIDE4 = 24
LEVELS = 4
SIDE5 = 12
SIDE6 = 6
SIDE7 = 3
IMAGES = 32


def feature_values(key, extent):
    noise_key, offset_key = jax.random.split(key, 2)
    places = jnp.arange(IMAGES, dtype=jnp.float32) / max(IMAGES - 1, 1)
    image_ramp = 1.0 + 2.0 * places
    noise_part = jnp.clip(jax.random.normal(noise_key, (IMAGES, extent, extent, CH), jnp.float32), -6.0, 6.0)
    offset = jax.random.uniform(offset_key, (IMAGES, 1, 1, CH), jnp.float32, -0.5, 1.0)
    values = image_ramp[:, None, None, None] * (noise_part + offset)
    return values.astype(jnp.bfloat16)


def draw_feat4(key, part):
    return feature_values(jax.random.fold_in(key, 4), SIDE4)


def draw_feat5(key, part):
    return feature_values(jax.random.fold_in(key, 5), SIDE5)


def draw_feat6(key, part):
    return feature_values(jax.random.fold_in(key, 6), SIDE6)


def draw_feat7(key, part):
    return feature_values(jax.random.fold_in(key, 7), SIDE7)


def place_ends(entries, own_key, smallest, top_value):
    longest = entries.shape.index(max(entries.shape))
    spots = []
    for shift in (0, 1):
        where = [jax.random.randint(jax.random.fold_in(own_key, axis), (), 0, length) for axis, length in enumerate(entries.shape)]
        where[longest] = (where[longest] + shift) % entries.shape[longest]
        spots.append(tuple(where))
    return entries.at[spots[0]].set(smallest).at[spots[1]].set(top_value)


def block_levels(stream_key, shape, shards, smallest, largest):
    level = 1.0
    for position, parts in shards:
        draws = jax.random.uniform(jax.random.fold_in(jax.random.fold_in(stream_key, 6), position), (parts,), jnp.float32, smallest / len(shards), largest / len(shards))
        level = level * jnp.repeat(jnp.exp(draws), shape[position] // parts).reshape((-1,) + (1,) * (len(shape) - 1 - position))
    return level


def bell_draw(key, dims, spread, bound, cuts=(), held_as=jnp.bfloat16):
    entries = jax.random.normal(key, dims, jnp.float32) * spread
    if len(cuts) > 0:
        entries = block_levels(key, dims, cuts, -0.22, 0.18) * entries
    return jnp.clip(entries, min=-bound, max=bound).astype(held_as)


def setup_inputs(seed: int = 0) -> dict:
    streams_of = jax.random.split(jax.random.key(seed), 14)
    feat4 = draw_feat4(jax.random.fold_in(streams_of[13], 71), 0)
    feat5 = draw_feat5(jax.random.fold_in(streams_of[13], 71), 0)
    feat6 = draw_feat6(jax.random.fold_in(streams_of[13], 71), 0)
    feat7 = draw_feat7(jax.random.fold_in(streams_of[13], 71), 0)
    out_grad4 = bell_draw(streams_of[4], (IMAGES, SIDE4, SIDE4, CH), 1.0, 6.0, ((0, 32),))
    out_grad5 = bell_draw(streams_of[5], (IMAGES, SIDE5, SIDE5, CH), 1.0, 6.0, ((0, 32),))
    out_grad6 = bell_draw(streams_of[6], (IMAGES, SIDE6, SIDE6, CH), 1.0, 6.0, ((0, 32),))
    out_grad7 = bell_draw(streams_of[7], (IMAGES, SIDE7, SIDE7, CH), 1.0, 6.0, ((0, 32),))
    conv_weight = bell_draw(streams_of[8], (3, 3, CH, CH), (9 * CH) ** -0.5, 0.125)
    bn_gain = jnp.clip(1.0 + 0.15 * jax.random.normal(streams_of[9], (LEVELS, CH), jnp.float32), 0.25, 1.75)
    bn_shift = jnp.clip(jax.random.uniform(streams_of[10], (LEVELS, CH), jnp.float32, -0.5, 0.5), -0.5, 0.5)
    heights = place_ends(jax.random.randint(streams_of[11], (IMAGES,), SIDE4 * 7, SIDE4 * 16 + 1), jax.random.fold_in(streams_of[11], 1), SIDE4 * 7, SIDE4 * 16).astype(jnp.int32)
    widths = place_ends(jax.random.randint(streams_of[12], (IMAGES,), SIDE4 * 7, SIDE4 * 16 + 1), jax.random.fold_in(streams_of[12], 1), SIDE4 * 7, SIDE4 * 16).astype(jnp.int32)
    return {"feat4": feat4, "feat5": feat5, "feat6": feat6, "feat7": feat7, "out_grad4": out_grad4, "out_grad5": out_grad5, "out_grad6": out_grad6, "out_grad7": out_grad7, "conv_weight": conv_weight, "bn_gain": bn_gain, "bn_shift": bn_shift, "heights": heights, "widths": widths}


EPSILON = 1e-05

def level_masks(heights, widths, stride, extent):
    row_limit = (heights + stride - 1) // stride
    col_limit = (widths + stride - 1) // stride
    places = jnp.arange(extent, dtype=jnp.int32)
    inside = jnp.logical_and(places[None, :, None] < row_limit[:, None, None], places[None, None, :] < col_limit[:, None, None])
    return inside.astype(jnp.float32)

def conv_image(padded, conv_weight, extent):
    summed = jnp.zeros((extent * extent, conv_weight.shape[3]), jnp.float32)
    for tap_row in range(3):
        for tap_col in range(3):
            window = padded[tap_row:tap_row + extent, tap_col:tap_col + extent, :].reshape(extent * extent, -1)
            summed = summed + jnp.dot(window, conv_weight[tap_row, tap_col], preferred_element_type=jnp.float32)
    return summed.reshape(extent, extent, -1)

def input_grad_image(padded_back, conv_weight, extent):
    summed = jnp.zeros((extent * extent, conv_weight.shape[2]), jnp.float32)
    for tap_row in range(3):
        for tap_col in range(3):
            window = padded_back[2 - tap_row:2 - tap_row + extent, 2 - tap_col:2 - tap_col + extent, :].reshape(extent * extent, -1)
            summed = summed + lax.dot_general(window, conv_weight[tap_row, tap_col], (((1,), (1,)), ((), ())), preferred_element_type=jnp.float32)
    return summed.reshape(extent, extent, -1)

def weight_grad_image(padded, back_grad, extent):
    flat_back = back_grad.reshape(extent * extent, -1)
    tap_terms = []
    for tap_row in range(3):
        for tap_col in range(3):
            window = padded[tap_row:tap_row + extent, tap_col:tap_col + extent, :].reshape(extent * extent, -1)
            tap_terms.append(lax.dot_general(window, flat_back, (((0,), (0,)), ((), ())), preferred_element_type=jnp.float32))
    return jnp.stack(tap_terms).reshape(3, 3, padded.shape[2], flat_back.shape[1])

def reference(feat4, feat5, feat6, feat7, out_grad4, out_grad5, out_grad6, out_grad7, conv_weight, bn_gain, bn_shift, heights, widths):
    features = (feat4, feat5, feat6, feat7)
    cotangents = (out_grad4, out_grad5, out_grad6, out_grad7)
    outputs = []
    input_grads = []
    gain_rows = []
    shift_rows = []
    weight_total = jnp.zeros(conv_weight.shape, jnp.float32)
    for level_index in range(4):
        feature = features[level_index]
        extent = feature.shape[1]
        valid_mask = level_masks(heights, widths, 16 * 2 ** level_index, extent)
        weighted = valid_mask[..., None]
        masked = feature * weighted.astype(feature.dtype)
        padded = jnp.pad(masked, ((0, 0), (1, 1), (1, 1), (0, 0)))
        conv_out = lax.map(partial(conv_image, conv_weight=conv_weight, extent=extent), padded)
        pixel_count = jnp.sum(valid_mask)
        mean_value = lax.optimization_barrier(jnp.sum(conv_out * weighted, axis=(0, 1, 2))) / pixel_count
        centered = conv_out - mean_value
        variance = lax.optimization_barrier(jnp.sum(weighted * centered * centered, axis=(0, 1, 2))) / pixel_count
        inverse = lax.rsqrt(variance + EPSILON)
        normed = centered * inverse
        shifted = bn_gain[level_index] * normed + bn_shift[level_index]
        sigmoid_value = jax.nn.sigmoid(shifted)
        outputs.append((weighted * shifted * sigmoid_value).astype(jnp.bfloat16))
        slope_term = weighted * cotangents[level_index].astype(jnp.float32) * sigmoid_value * (1.0 + shifted * (1.0 - sigmoid_value))
        shift_sum = lax.optimization_barrier(jnp.sum(slope_term, axis=(0, 1, 2)))
        gain_sum = lax.optimization_barrier(jnp.sum(slope_term * normed, axis=(0, 1, 2)))
        back_grad = (weighted * (bn_gain[level_index] * inverse) * (slope_term - shift_sum / pixel_count - normed * (gain_sum / pixel_count))).astype(jnp.bfloat16)

        def add_image(carry_total, operands, extent=extent):
            return (carry_total + weight_grad_image(operands[0], operands[1], extent), None)
        weight_total, unused = lax.scan(add_image, weight_total, (padded, back_grad))
        padded_back = jnp.pad(back_grad, ((0, 0), (1, 1), (1, 1), (0, 0)))
        input_part = lax.map(partial(input_grad_image, conv_weight=conv_weight, extent=extent), padded_back)
        input_grads.append((weighted * input_part).astype(jnp.bfloat16))
        gain_rows.append(gain_sum)
        shift_rows.append(shift_sum)
    return (outputs[0], outputs[1], outputs[2], outputs[3], input_grads[0], input_grads[1], input_grads[2], input_grads[3], weight_total / IMAGES, jnp.stack(gain_rows) / IMAGES, jnp.stack(shift_rows) / IMAGES)
```

```python
import jax
import jax.numpy as jnp
from jax import lax
from jax.sharding import PartitionSpec as P

EPSILON = 1e-05


def level_mask(heights, widths, stride, extent):
    row_limit = (heights[0] + stride - 1) // stride
    col_limit = (widths[0] + stride - 1) // stride
    row_place = lax.broadcasted_iota(jnp.int32, (extent, extent), 0)
    col_place = lax.broadcasted_iota(jnp.int32, (extent, extent), 1)
    inside = jnp.logical_and(row_place < row_limit, col_place < col_limit)
    return (inside.astype(jnp.float32), row_limit)


def conv_rows(padded, conv_weight, start_row, row_count, extent):
    summed = jnp.zeros((row_count * extent, conv_weight.shape[3]), jnp.float32)
    for tap_row in range(3):
        for tap_col in range(3):
            window = lax.dynamic_slice_in_dim(padded, start_row + tap_row, row_count, 0)[
                :, tap_col : tap_col + extent, :
            ]
            summed = summed + jnp.dot(
                window.reshape(row_count * extent, -1),
                conv_weight[tap_row, tap_col],
                preferred_element_type=jnp.float32,
            )
    return summed.reshape(row_count, extent, -1)


def input_grad_rows(padded_back, conv_weight, start_row, row_count, extent):
    summed = jnp.zeros((row_count * extent, conv_weight.shape[2]), jnp.float32)
    for tap_row in range(3):
        for tap_col in range(3):
            window = lax.dynamic_slice_in_dim(padded_back, start_row + 2 - tap_row, row_count, 0)[
                :, 2 - tap_col : 2 - tap_col + extent, :
            ]
            summed = summed + lax.dot_general(
                window.reshape(row_count * extent, -1),
                conv_weight[tap_row, tap_col],
                (((1,), (1,)), ((), ())),
                preferred_element_type=jnp.float32,
            )
    return summed.reshape(row_count, extent, -1)


def weight_grad_rows(padded, back_rows, start_row, row_count, extent):
    flat_back = back_rows.reshape(row_count * extent, -1)
    tap_terms = []
    for tap_row in range(3):
        for tap_col in range(3):
            window = lax.dynamic_slice_in_dim(padded, start_row + tap_row, row_count, 0)[
                :, tap_col : tap_col + extent, :
            ]
            tap_terms.append(
                lax.dot_general(
                    window.reshape(row_count * extent, -1),
                    flat_back,
                    (((0,), (0,)), ((), ())),
                    preferred_element_type=jnp.float32,
                )
            )
    return jnp.stack(tap_terms).reshape(3, 3, padded.shape[2], flat_back.shape[1])


def forward_conv(padded, conv_weight, extent):
    conv_out = conv_rows(padded, conv_weight, 0, extent, extent)
    return conv_out


def backward_conv(padded, back_grad, conv_weight, extent):
    padded_back = jnp.pad(back_grad, ((1, 1), (1, 1), (0, 0)))
    weight_part = weight_grad_rows(padded, back_grad, 0, extent, extent)
    input_part = input_grad_rows(padded_back, conv_weight, 0, extent, extent)
    return (weight_part, input_part)


def layout():
    group_size = lax.axis_size("group")
    wide_size = lax.axis_size("wide")
    core_size = 2 if group_size % 2 == 0 else 1
    col_size = group_size // core_size
    row_size = col_size if wide_size % col_size == 0 else 1
    return (core_size, col_size, row_size, wide_size // row_size)


def places():
    core_size, col_size, row_size, deep_size = layout()
    group_index = lax.axis_index("group")
    wide_index = lax.axis_index("wide")
    plane_index = (wide_index % row_size) * col_size + group_index // core_size
    return (group_index % core_size, plane_index, wide_index // row_size)


def exchange(values, core_step, plane_step, deep_step):
    core_size, col_size, row_size, deep_size = layout()
    plane_size = col_size * row_size
    pairs = []
    for deep in range(deep_size):
        for plane in range(plane_size):
            for core in range(core_size):
                ends = []
                for core_end, plane_end, deep_end in (
                    (core, plane, deep),
                    (
                        (core + core_step) % core_size,
                        (plane + plane_step) % plane_size,
                        (deep + deep_step) % deep_size,
                    ),
                ):
                    wide_index = deep_end * row_size + plane_end // col_size
                    group_index = (plane_end % col_size) * core_size + core_end
                    ends.append(wide_index * col_size * core_size + group_index)
                pairs.append(tuple(ends))
    return lax.ppermute(values, ("wide", "group"), pairs)


def piece(values, index, count):
    rows = values.shape[0] // count
    return lax.dynamic_slice_in_dim(values, index * rows, rows, 0)


def scatter_stage(values, place, size, send):
    arrived = [send(piece(values, (place + step) % size, size), step) for step in range(1, size)]
    total = piece(values, place, size)
    for part in arrived:
        total = total + part
    return total


def gather_stage(values, place, size, send):
    rows = values.shape[0]
    arrived = [values] + [send(values, step) for step in range(1, size)]
    whole = jnp.zeros((rows * size,) + values.shape[1:], values.dtype)
    for step, part in enumerate(arrived):
        whole = lax.dynamic_update_slice_in_dim(whole, part, ((place - step) % size) * rows, 0)
    return whole


def combine_stats(values):
    devices = lax.axis_size("wide") * lax.axis_size("group")
    flat = jnp.concatenate([jnp.ravel(value) for value in values])
    width = -(-flat.shape[0] // 1024) * 1024
    packed = jnp.pad(flat, (0, width - flat.shape[0])).reshape(-1, 128)
    spread = jnp.broadcast_to(packed[None], (devices,) + packed.shape)
    total = jnp.sum(lax.all_to_all(spread, ("wide", "group"), 0, 0), axis=0).reshape(-1)
    results = []
    start = 0
    for value in values:
        results.append(total[start : start + value.size].reshape(value.shape))
        start += value.size
    return tuple(results)


def combine_grads(values):
    core_size, col_size, row_size, deep_size = layout()
    core, plane, deep = places()
    stages = (
        (core, core_size, lambda part, step: exchange(part, step, 0, 0)),
        (plane, col_size * row_size, lambda part, step: exchange(part, 0, step, 0)),
        (deep, deep_size, lambda part, step: exchange(part, 0, 0, step)),
    )
    total = values.reshape(-1, values.shape[-1])
    for place, size, send in stages:
        total = scatter_stage(total, place, size, send)
    for place, size, send in reversed(stages):
        total = gather_stage(total, place, size, send)
    return total.reshape(values.shape)


def shards(
    feat4,
    feat5,
    feat6,
    feat7,
    out_grad4,
    out_grad5,
    out_grad6,
    out_grad7,
    conv_weight,
    bn_gain,
    bn_shift,
    heights,
    widths,
):
    features = (feat4, feat5, feat6, feat7)
    cotangents = (out_grad4, out_grad5, out_grad6, out_grad7)
    devices = lax.axis_size("wide") * lax.axis_size("group")
    levels = []
    for level_index in range(4):
        feature = features[level_index][0]
        extent = feature.shape[0]
        valid_mask, row_limit = level_mask(heights, widths, 16 * 2**level_index, extent)
        weighted = valid_mask[:, :, None]
        padded = jnp.pad(feature * weighted.astype(feature.dtype), ((1, 1), (1, 1), (0, 0)))
        conv_out = forward_conv(padded, conv_weight, extent)
        levels.append((valid_mask, row_limit, weighted, padded, conv_out))
    moments = []
    local_sums = jnp.stack(
        [jnp.sum(level_entry[4] * level_entry[2], axis=(0, 1)) for level_entry in levels]
    )
    local_squares = jnp.stack(
        [
            jnp.sum(level_entry[2] * level_entry[4] * level_entry[4], axis=(0, 1))
            for level_entry in levels
        ]
    )
    local_counts = jnp.stack([jnp.sum(level_entry[0]) for level_entry in levels])
    moment_sums, squares, counts = combine_stats((local_sums, local_squares, local_counts))
    for level_index in range(4):
        pixel_count = counts[level_index]
        mean_value = moment_sums[level_index] / pixel_count
        moments.append(
            (pixel_count, mean_value, squares[level_index] / pixel_count - mean_value * mean_value)
        )
    finals = []
    for level_index in range(4):
        valid_mask, row_limit, weighted, padded, conv_out = levels[level_index]
        pixel_count, mean_value, variance = moments[level_index]
        inverse = lax.rsqrt(variance + EPSILON)
        normed = (conv_out - mean_value) * inverse
        shifted = bn_gain[level_index] * normed + bn_shift[level_index]
        sigmoid_value = jax.nn.sigmoid(shifted)
        output = (weighted * shifted * sigmoid_value).astype(jnp.bfloat16)
        slope_term = (
            weighted
            * cotangents[level_index][0].astype(jnp.float32)
            * sigmoid_value
            * (1.0 + shifted * (1.0 - sigmoid_value))
        )
        finals.append((output, normed, inverse, slope_term))
    shift_local = jnp.stack([jnp.sum(final_entry[3], axis=(0, 1)) for final_entry in finals])
    gain_local = jnp.stack(
        [jnp.sum(final_entry[3] * final_entry[1], axis=(0, 1)) for final_entry in finals]
    )
    shift_rows, gain_rows = combine_stats((shift_local, gain_local))
    back_sums = [(shift_rows[level_index], gain_rows[level_index]) for level_index in range(4)]
    weight_local = jnp.zeros(conv_weight.shape, jnp.float32)
    outputs = []
    input_grads = []
    shift_list = []
    gain_list = []
    for level_index in range(4):
        valid_mask, row_limit, weighted, padded, conv_out = levels[level_index]
        pixel_count, mean_value, variance = moments[level_index]
        output, normed, inverse, slope_term = finals[level_index]
        shift_sum, gain_sum = back_sums[level_index]
        extent = conv_out.shape[0]
        back_grad = (
            weighted
            * (bn_gain[level_index] * inverse)
            * (slope_term - shift_sum / pixel_count - normed * (gain_sum / pixel_count))
        ).astype(jnp.bfloat16)
        weight_part, input_part = backward_conv(padded, back_grad, conv_weight, extent)
        weight_local = weight_local + weight_part
        input_grads.append((weighted * input_part).astype(jnp.bfloat16)[None])
        outputs.append(output[None])
        shift_list.append(shift_sum)
        gain_list.append(gain_sum)
    weight_total = combine_grads(weight_local)
    return (
        outputs[0],
        outputs[1],
        outputs[2],
        outputs[3],
        input_grads[0],
        input_grads[1],
        input_grads[2],
        input_grads[3],
        weight_total / devices,
        jnp.stack(gain_list) / devices,
        jnp.stack(shift_list) / devices,
    )


def solution(mesh):
    placed = (
        P(("wide", "group"), None, None, None),
        P(("wide", "group"), None, None, None),
        P(("wide", "group"), None, None, None),
        P(("wide", "group"), None, None, None),
        P(("wide", "group"), None, None, None),
        P(("wide", "group"), None, None, None),
        P(("wide", "group"), None, None, None),
        P(("wide", "group"), None, None, None),
        P(),
        P(),
        P(),
        P(("wide", "group")),
        P(("wide", "group")),
    )
    return jax.shard_map(
        shards,
        mesh=mesh,
        in_specs=placed,
        out_specs=(
            P(("wide", "group"), None, None, None),
            P(("wide", "group"), None, None, None),
            P(("wide", "group"), None, None, None),
            P(("wide", "group"), None, None, None),
            P(("wide", "group"), None, None, None),
            P(("wide", "group"), None, None, None),
            P(("wide", "group"), None, None, None),
            P(("wide", "group"), None, None, None),
            P(),
            P(),
            P(),
        ),
        check_vma=False,
    )
```

```python
from functools import partial

import jax
import jax.numpy as jnp
from jax import lax
from jax.experimental import pallas as pl
from jax.experimental.pallas import tpu as pltpu
from jax.sharding import PartitionSpec as P

EPSILON = 1e-05
PITCH = 32
STRIDE = 16
VMEM = pl.BlockSpec(memory_space=pltpu.VMEM)
SMEM = pl.BlockSpec(memory_space=pltpu.SMEM)


def canvas_spots(extents):
    spots = [(1, 0, extents[0])]
    column = 0
    for extent in extents[1:]:
        spots.append((extents[0] + 2, column, extent))
        column += -(-(extent + 1) // 8) * 8
    rows = extents[0] + extents[1] + 3
    assert column <= PITCH and extents[0] < PITCH
    return tuple(spots), rows


def level_limits(heights_ref, widths_ref, level_index, extent):
    stride = STRIDE * 2**level_index
    row_limit = jnp.minimum((heights_ref[0] + (stride - 1)) // stride, extent)
    col_limit = jnp.minimum((widths_ref[0] + (stride - 1)) // stride, extent)
    return (row_limit, col_limit)


def inside_mask(limits, shape):
    row_place = lax.broadcasted_iota(jnp.int32, shape, 0)
    col_place = lax.broadcasted_iota(jnp.int32, shape, 1)
    return jnp.logical_and(row_place < limits[0], col_place < limits[1])


def put_row(ref, row, vector):
    for part in range(vector.shape[1] // 128):
        ref[row + part : row + part + 1, :] = vector[:, part * 128 : (part + 1) * 128]


def get_row(packed, level_index, parts):
    rows = [packed[level_index * parts + part : level_index * parts + part + 1, :] for part in range(parts)]
    return jnp.concatenate(rows, axis=1)


def spread_columns(source, target, rows, channels):
    flat = source[...].reshape(rows * PITCH, channels)
    target[:, 0:channels] = pltpu.roll(flat, 1, 0).astype(jnp.bfloat16)
    target[:, channels : 2 * channels] = flat.astype(jnp.bfloat16)
    target[:, 2 * channels :] = pltpu.roll(flat, rows * PITCH - 1, 0).astype(jnp.bfloat16)


def forward_kernel(
    spots,
    rows,
    heights_ref,
    widths_ref,
    feat4_ref,
    feat5_ref,
    feat6_ref,
    feat7_ref,
    weight_ref,
    spread_ref,
    conv_ref,
    payload_ref,
    canvas,
    packed,
):
    channels = weight_ref.shape[2]
    parts = channels // 128
    canvas[...] = jnp.zeros_like(canvas)
    for level_index, (feat_ref, (row, column, extent)) in enumerate(
        zip((feat4_ref, feat5_ref, feat6_ref, feat7_ref), spots)
    ):
        limits = level_limits(heights_ref, widths_ref, level_index, extent)
        values = feat_ref[0].astype(jnp.float32)
        inside = inside_mask(limits, values.shape)
        canvas[row : row + extent, column : column + extent, :] = jnp.where(inside, values, 0.0)
    spread_columns(canvas, spread_ref, rows, channels)
    body = (rows - 2) * PITCH
    summed = jnp.zeros((body, channels), jnp.float32)
    for tap_row in range(3):
        summed = summed + jnp.dot(
            spread_ref[tap_row * PITCH : tap_row * PITCH + body, :],
            weight_ref[tap_row],
            preferred_element_type=jnp.float32,
        )
    conv_ref[...] = summed.reshape(rows - 2, PITCH, channels)
    for level_index, (row, column, extent) in enumerate(spots):
        limits = level_limits(heights_ref, widths_ref, level_index, extent)
        conv_out = conv_ref[row - 1 : row - 1 + extent, column : column + extent, :]
        inside = inside_mask(limits, conv_out.shape)
        count = (limits[0] * limits[1]).astype(jnp.float32)
        total = jnp.sum(jnp.where(inside, conv_out, 0.0), axis=(0, 1)).reshape(1, channels)
        centered = jnp.where(inside, conv_out - total / count, 0.0)
        spread = jnp.sum(centered * centered, axis=(0, 1)).reshape(1, channels)
        put_row(packed, level_index * parts, total)
        put_row(packed, (4 + level_index) * parts, spread)
        put_row(packed, (8 + level_index) * parts, jnp.full((1, channels), count, jnp.float32))
    payload_ref[...] = jnp.broadcast_to(packed[...][None], payload_ref.shape)


def middle_kernel(
    spots,
    heights_ref,
    widths_ref,
    gathered_ref,
    conv_ref,
    cot4_ref,
    cot5_ref,
    cot6_ref,
    cot7_ref,
    gain_ref,
    bias_ref,
    out4_ref,
    out5_ref,
    out6_ref,
    out7_ref,
    slope_ref,
    moments_ref,
    payload_ref,
    packed,
):
    channels = gain_ref.shape[1]
    parts = channels // 128
    block = 4 * parts
    sums = gathered_ref[:, 0:block, :]
    spreads = gathered_ref[:, block : 2 * block, :]
    counts = gathered_ref[:, 2 * block : 3 * block, :]
    total_count = jnp.sum(counts, axis=0)
    mean_rows = jnp.sum(sums, axis=0) / total_count
    offset = sums / counts - mean_rows[None]
    variance = jnp.sum(spreads + counts * offset * offset, axis=0) / total_count
    inverse_rows = lax.rsqrt(variance + EPSILON)
    moments_ref[0:block, :] = mean_rows
    moments_ref[block : 2 * block, :] = inverse_rows
    moments_ref[2 * block : 3 * block, :] = total_count
    slope_ref[...] = jnp.zeros_like(slope_ref)
    for level_index, (cot_ref, out_ref, (row, column, extent)) in enumerate(
        zip((cot4_ref, cot5_ref, cot6_ref, cot7_ref), (out4_ref, out5_ref, out6_ref, out7_ref), spots)
    ):
        limits = level_limits(heights_ref, widths_ref, level_index, extent)
        mean_value = get_row(mean_rows, level_index, parts)[None]
        inverse = get_row(inverse_rows, level_index, parts)[None]
        gain = gain_ref[level_index : level_index + 1, :][None]
        bias = bias_ref[level_index : level_index + 1, :][None]
        conv_out = conv_ref[row - 1 : row - 1 + extent, column : column + extent, :]
        inside = inside_mask(limits, conv_out.shape)
        normed = (conv_out - mean_value) * inverse
        shifted = gain * normed + bias
        sigmoid_value = 1.0 / (1.0 + jnp.exp(-shifted))
        out_ref[0] = jnp.where(inside, shifted * sigmoid_value, 0.0).astype(jnp.bfloat16)
        slope = cot_ref[0].astype(jnp.float32) * sigmoid_value * (1.0 + shifted * (1.0 - sigmoid_value))
        slope = jnp.where(inside, slope, 0.0)
        slope_ref[row - 1 : row - 1 + extent, column : column + extent, :] = slope
        put_row(packed, level_index * parts, jnp.sum(slope, axis=(0, 1)).reshape(1, channels))
        put_row(packed, (4 + level_index) * parts, jnp.sum(slope * normed, axis=(0, 1)).reshape(1, channels))
    payload_ref[...] = jnp.broadcast_to(packed[...][None], payload_ref.shape)


def weight_grad_rows(spread_ref, turned, first, rows, body, channels, target_ref):
    step = channels // 2
    for start in range(0, rows, step):
        place = first + start
        tap_row = place // (3 * channels)
        lane = pl.multiple_of(place - tap_row * 3 * channels, 128)
        window = spread_ref[pl.ds(pl.multiple_of(tap_row * PITCH, PITCH), body), pl.ds(lane, step)]
        target_ref[start : start + step, :] = lax.dot_general(
            window, turned, (((0,), (0,)), ((), ())), preferred_element_type=jnp.float32
        )


def back_kernel(
    spots,
    core_size,
    devices,
    heights_ref,
    widths_ref,
    core_ref,
    gathered_ref,
    conv_ref,
    slope_ref,
    moments_ref,
    gain_ref,
    spread_ref,
    back_ref,
    send_ref,
    d_gain_ref,
    d_shift_ref,
):
    channels = gain_ref.shape[1]
    parts = channels // 128
    block = 4 * parts
    shift_rows = jnp.sum(gathered_ref[:, 0:block, :], axis=0)
    gain_rows = jnp.sum(gathered_ref[:, block : 2 * block, :], axis=0)
    back_ref[...] = jnp.zeros_like(back_ref)
    for level_index, (row, column, extent) in enumerate(spots):
        limits = level_limits(heights_ref, widths_ref, level_index, extent)
        mean_value = get_row(moments_ref[0:block, :], level_index, parts)[None]
        inverse = get_row(moments_ref[block : 2 * block, :], level_index, parts)[None]
        count = get_row(moments_ref[2 * block : 3 * block, :], level_index, parts)[None]
        shift_sum = get_row(shift_rows, level_index, parts)
        gain_sum = get_row(gain_rows, level_index, parts)
        d_gain_ref[level_index : level_index + 1, :] = gain_sum / devices
        d_shift_ref[level_index : level_index + 1, :] = shift_sum / devices
        gain = gain_ref[level_index : level_index + 1, :][None]
        conv_out = conv_ref[row - 1 : row - 1 + extent, column : column + extent, :]
        slope = slope_ref[row - 1 : row - 1 + extent, column : column + extent, :]
        inside = inside_mask(limits, conv_out.shape)
        normed = (conv_out - mean_value) * inverse
        back = (gain * inverse) * (slope - shift_sum[None] / count - normed * (gain_sum[None] / count))
        back_ref[row : row + extent, column : column + extent, :] = jnp.where(inside, back, 0.0)
    rows = back_ref.shape[0]
    body = (rows - 2) * PITCH
    turned = back_ref[1 : rows - 1].reshape(body, channels).astype(jnp.bfloat16)
    half = send_ref.shape[0]
    first = (core_size - 1 - core_ref[0]) * half
    weight_grad_rows(spread_ref, turned, first, half, body, channels, send_ref)


def keep_kernel(core_ref, back_ref, spread_ref, keep_ref):
    rows, pitch, channels = back_ref.shape
    body = (rows - 2) * PITCH
    turned = back_ref[1 : rows - 1].reshape(body, channels).astype(jnp.bfloat16)
    half = keep_ref.shape[0]
    weight_grad_rows(spread_ref, turned, core_ref[0] * half, half, body, channels, keep_ref)


def input_grad_kernel(
    spots,
    heights_ref,
    widths_ref,
    back_ref,
    weight_ref,
    d_feat4_ref,
    d_feat5_ref,
    d_feat6_ref,
    d_feat7_ref,
    spread,
    summed,
):
    rows, pitch, channels = back_ref.shape
    body = (rows - 2) * PITCH
    spread_columns(back_ref, spread, rows, channels)
    total = jnp.zeros((body, channels), jnp.float32)
    for tap_row in range(3):
        for tap_col in range(3):
            start = (2 - tap_row) * PITCH
            lane = (2 - tap_col) * channels
            total = total + lax.dot_general(
                spread[start : start + body, lane : lane + channels],
                weight_ref[tap_row, tap_col * channels : (tap_col + 1) * channels, :],
                (((1,), (1,)), ((), ())),
                preferred_element_type=jnp.float32,
            )
    summed[...] = total.reshape(rows - 2, PITCH, channels)
    for level_index, (target_ref, (row, column, extent)) in enumerate(
        zip((d_feat4_ref, d_feat5_ref, d_feat6_ref, d_feat7_ref), spots)
    ):
        limits = level_limits(heights_ref, widths_ref, level_index, extent)
        values = summed[row - 1 : row - 1 + extent, column : column + extent, :]
        target_ref[0] = jnp.where(inside_mask(limits, values.shape), values, 0.0).astype(jnp.bfloat16)


def call(kernel, name, outputs, in_specs, scratch=(), flops=0, moved=0):
    return pl.pallas_call(
        kernel,
        out_shape=outputs,
        in_specs=in_specs,
        out_specs=jax.tree.map(lambda leaf: VMEM, outputs),
        scratch_shapes=scratch,
        compiler_params=pltpu.CompilerParams(vmem_limit_bytes=30 * 1024 * 1024),
        cost_estimate=pl.CostEstimate(flops=flops, bytes_accessed=moved, transcendentals=0),
        name=name,
    )


def layout():
    group_size = lax.axis_size("group")
    wide_size = lax.axis_size("wide")
    core_size = 2 if group_size % 2 == 0 else 1
    col_size = group_size // core_size
    row_size = col_size if wide_size % col_size == 0 else 1
    return (core_size, col_size, row_size, wide_size // row_size)


def places():
    core_size, col_size, row_size, deep_size = layout()
    group_index = lax.axis_index("group")
    wide_index = lax.axis_index("wide")
    plane_index = (wide_index % row_size) * col_size + group_index // core_size
    return (group_index % core_size, plane_index, wide_index // row_size)


def exchange(values, core_step, plane_step, deep_step):
    core_size, col_size, row_size, deep_size = layout()
    plane_size = col_size * row_size
    pairs = []
    for deep in range(deep_size):
        for plane in range(plane_size):
            for core in range(core_size):
                ends = []
                for core_end, plane_end, deep_end in (
                    (core, plane, deep),
                    (
                        (core + core_step) % core_size,
                        (plane + plane_step) % plane_size,
                        (deep + deep_step) % deep_size,
                    ),
                ):
                    wide_index = deep_end * row_size + plane_end // col_size
                    group_index = (plane_end % col_size) * core_size + core_end
                    ends.append(wide_index * col_size * core_size + group_index)
                pairs.append(tuple(ends))
    return lax.ppermute(values, ("wide", "group"), pairs)


def piece(values, index, count):
    rows = values.shape[0] // count
    return lax.dynamic_slice_in_dim(values, index * rows, rows, 0)


def scatter_stage(values, place, size, send):
    arrived = [send(piece(values, (place + step) % size, size), step) for step in range(1, size)]
    total = piece(values, place, size)
    for part in arrived:
        total = total + part
    return total


def gather_stage(values, place, size, send):
    rows = values.shape[0]
    arrived = [values] + [send(values, step) for step in range(1, size)]
    whole = jnp.zeros((rows * size,) + values.shape[1:], values.dtype)
    for step, part in enumerate(arrived):
        whole = lax.dynamic_update_slice_in_dim(whole, part, ((place - step) % size) * rows, 0)
    return whole


def swap_stats(payload):
    return lax.all_to_all(payload, ("wide", "group"), 0, 0)


def combine_grads(keep, send, devices):
    core_size, col_size, row_size, deep_size = layout()
    core, plane, deep = places()
    core_send = lambda part, step: exchange(part, step, 0, 0)
    stages = (
        (plane, col_size * row_size, lambda part, step: exchange(part, 0, step, 0)),
        (deep, deep_size, lambda part, step: exchange(part, 0, 0, step)),
    )
    total = keep
    if core_size > 1:
        total = total + core_send(send, 1)
    for place, size, send_part in stages:
        total = scatter_stage(total, place, size, send_part)
    total = total / devices
    for place, size, send_part in reversed(stages):
        total = gather_stage(total, place, size, send_part)
    return gather_stage(total, core, core_size, core_send)


def struct(shape, dtype=jnp.float32):
    return jax.ShapeDtypeStruct(shape, dtype)


def shards(
    feat4,
    feat5,
    feat6,
    feat7,
    out_grad4,
    out_grad5,
    out_grad6,
    out_grad7,
    conv_weight,
    bn_gain,
    bn_shift,
    heights,
    widths,
):
    features = (feat4, feat5, feat6, feat7)
    cotangents = (out_grad4, out_grad5, out_grad6, out_grad7)
    devices = lax.axis_size("wide") * lax.axis_size("group")
    core_size = layout()[0]
    core = places()[0].astype(jnp.int32).reshape(1)
    channels = conv_weight.shape[2]
    parts = channels // 128
    spots, rows = canvas_spots(tuple(feature.shape[1] for feature in features))
    body = (rows - 2) * PITCH
    folded = conv_weight.reshape(3, 3 * channels, channels)
    work = 2 * body * 9 * channels * channels
    half = 9 * channels // core_size

    spread, conv_out, payload = call(
        partial(forward_kernel, spots, rows),
        "forward",
        (
            struct((rows * PITCH, 3 * channels), jnp.bfloat16),
            struct((rows - 2, PITCH, channels)),
            struct((devices, 12 * parts, 128)),
        ),
        [SMEM, SMEM] + [VMEM] * 5,
        [pltpu.VMEM((rows, PITCH, channels), jnp.float32), pltpu.VMEM((12 * parts, 128), jnp.float32)],
        flops=work,
    )(heights, widths, *features, folded)
    gathered = swap_stats(payload)
    out4, out5, out6, out7, slope, moments, payload = call(
        partial(middle_kernel, spots),
        "middle",
        tuple(struct(feature.shape, jnp.bfloat16) for feature in features)
        + (
            struct((rows - 2, PITCH, channels)),
            struct((12 * parts, 128)),
            struct((devices, 8 * parts, 128)),
        ),
        [SMEM, SMEM] + [VMEM] * 8,
        [pltpu.VMEM((8 * parts, 128), jnp.float32)],
        flops=body * channels * 100,
    )(heights, widths, gathered, conv_out, *cotangents, bn_gain, bn_shift)
    gathered = swap_stats(payload)
    back, send, d_gain, d_shift = call(
        partial(back_kernel, spots, core_size, devices),
        "back",
        (
            struct((rows, PITCH, channels)),
            struct((half, channels)),
            struct(bn_gain.shape),
            struct(bn_gain.shape),
        ),
        [SMEM] * 3 + [VMEM] * 6,
        flops=work // core_size,
    )(heights, widths, core, gathered, conv_out, slope, moments, bn_gain, spread)
    keep = call(
        keep_kernel,
        "keep",
        struct((half, channels)),
        [SMEM, VMEM, VMEM],
        flops=work // core_size,
    )(core, back, spread)
    input_grads = call(
        partial(input_grad_kernel, spots),
        "input_grad",
        tuple(struct(feature.shape, jnp.bfloat16) for feature in features),
        [SMEM, SMEM, VMEM, VMEM],
        [
            pltpu.VMEM((rows * PITCH, 3 * channels), jnp.bfloat16),
            pltpu.VMEM((rows - 2, PITCH, channels), jnp.float32),
        ],
        flops=work,
    )(heights, widths, back, folded)
    weight_total = combine_grads(keep, send, devices).reshape(conv_weight.shape)
    return (out4, out5, out6, out7, *input_grads, weight_total, d_gain, d_shift)


def solution(mesh):
    placed = (
        P(("wide", "group"), None, None, None),
        P(("wide", "group"), None, None, None),
        P(("wide", "group"), None, None, None),
        P(("wide", "group"), None, None, None),
        P(("wide", "group"), None, None, None),
        P(("wide", "group"), None, None, None),
        P(("wide", "group"), None, None, None),
        P(("wide", "group"), None, None, None),
        P(),
        P(),
        P(),
        P(("wide", "group")),
        P(("wide", "group")),
    )
    return jax.shard_map(
        shards,
        mesh=mesh,
        in_specs=placed,
        out_specs=(
            P(("wide", "group"), None, None, None),
            P(("wide", "group"), None, None, None),
            P(("wide", "group"), None, None, None),
            P(("wide", "group"), None, None, None),
            P(("wide", "group"), None, None, None),
            P(("wide", "group"), None, None, None),
            P(("wide", "group"), None, None, None),
            P(("wide", "group"), None, None, None),
            P(),
            P(),
            P(),
        ),
        check_vma=False,
    )
```

```python
from functools import partial

import jax
import jax.numpy as jnp
from jax import lax
from jax.experimental import pallas as pl
from jax.experimental.pallas import tpu as pltpu
from jax.sharding import PartitionSpec as P

EPSILON = 1e-05
PITCH = 32
STRIDE = 16
VMEM = pl.BlockSpec(memory_space=pltpu.VMEM)
HBM = pl.BlockSpec(memory_space=pltpu.HBM)


def canvas_spots(extents):
    spots = [(1, 0, extents[0])]
    column = 0
    for extent in extents[1:]:
        spots.append((extents[0] + 2, column, extent))
        column += -(-(extent + 1) // 8) * 8
    rows = extents[0] + extents[1] + 3
    assert column <= PITCH and extents[0] < PITCH
    return tuple(spots), rows


def level_limits(sizes_ref, level_index, extent):
    stride = STRIDE * 2**level_index
    shift = stride.bit_length() - 1
    limits = []
    for line in range(2):
        pixels = sizes_ref[line : line + 1, 0:1].reshape(1, 1, 1)
        limits.append(jnp.minimum(lax.shift_right_arithmetic(pixels + (stride - 1), shift), extent))
    return tuple(limits)


def inside_mask(limits, shape):
    row_place = lax.broadcasted_iota(jnp.int32, shape, 0)
    col_place = lax.broadcasted_iota(jnp.int32, shape, 1)
    return jnp.logical_and(row_place < limits[0], col_place < limits[1])


def put_row(ref, row, vector):
    for part in range(vector.shape[1] // 128):
        ref[row + part : row + part + 1, :] = vector[:, part * 128 : (part + 1) * 128]


def get_row(packed, level_index, parts):
    rows = [packed[level_index * parts + part : level_index * parts + part + 1, :] for part in range(parts)]
    return jnp.concatenate(rows, axis=1)


def spread_columns(flat, target):
    cells, channels = flat.shape
    target[:, 0:channels] = pltpu.roll(flat, 1, 0).astype(jnp.bfloat16)
    target[:, channels : 2 * channels] = flat.astype(jnp.bfloat16)
    target[:, 2 * channels :] = pltpu.roll(flat, cells - 1, 0).astype(jnp.bfloat16)


def forward_kernel(spots, rows, *refs):
    sizes, *features_in = refs[0:5]
    weight_in, spread_ref, conv_ref, payload_ref, canvas, packed, weight_ref, *feature_refs = refs[5:16]
    semaphores = refs[16]
    copies = [
        pltpu.make_async_copy(source, target, semaphores.at[place])
        for place, (source, target) in enumerate(
            zip(
                (*features_in, weight_in),
                (*feature_refs, weight_ref),
            )
        )
    ]
    for copy in copies:
        copy.start()
    channels = weight_ref.shape[2]
    parts = channels // 128
    canvas[...] = jnp.zeros_like(canvas)
    for copy in copies[:-1]:
        copy.wait()
    for level_index, (feat_ref, (row, column, extent)) in enumerate(zip(feature_refs, spots)):
        limits = level_limits(sizes, level_index, extent)
        values = feat_ref[0].astype(jnp.float32)
        inside = inside_mask(limits, values.shape)
        canvas[row : row + extent, column : column + extent, :] = jnp.where(inside, values, 0.0)
    spread_columns(canvas[...].reshape(rows * PITCH, channels), spread_ref)
    body = (rows - 2) * PITCH
    copies[-1].wait()
    summed = jnp.zeros((body, channels), jnp.float32)
    for tap_row in range(3):
        summed = summed + jnp.dot(
            spread_ref[tap_row * PITCH : tap_row * PITCH + body, :],
            weight_ref[tap_row],
            preferred_element_type=jnp.float32,
        )
    conv_ref[...] = summed.reshape(rows - 2, PITCH, channels)
    for level_index, (row, column, extent) in enumerate(spots):
        limits = level_limits(sizes, level_index, extent)
        conv_out = conv_ref[row - 1 : row - 1 + extent, column : column + extent, :]
        inside = inside_mask(limits, conv_out.shape)
        count = (limits[0] * limits[1]).astype(jnp.float32).reshape(1, 1)
        total = jnp.sum(jnp.where(inside, conv_out, 0.0), axis=(0, 1)).reshape(1, channels)
        centered = jnp.where(inside, conv_out - total / count, 0.0)
        spread = jnp.sum(centered * centered, axis=(0, 1)).reshape(1, channels)
        put_row(packed, level_index * parts, total)
        put_row(packed, (4 + level_index) * parts, spread)
        put_row(packed, (8 + level_index) * parts, jnp.broadcast_to(count, (1, channels)))
    payload_ref[...] = jnp.broadcast_to(packed[...][None], payload_ref.shape)


def normalized(spots, level_index, conv_ref, moments_ref, gain_ref, bias_ref):
    parts = gain_ref.shape[1] // 128
    block = 4 * parts
    row, column, extent = spots[level_index]
    mean_value = get_row(moments_ref[0:block, :], level_index, parts)[None]
    inverse = get_row(moments_ref[block : 2 * block, :], level_index, parts)[None]
    gain = gain_ref[level_index : level_index + 1, :][None]
    bias = bias_ref[level_index : level_index + 1, :][None]
    conv_out = conv_ref[row - 1 : row - 1 + extent, column : column + extent, :]
    normed = (conv_out - mean_value) * inverse
    return (normed, gain * normed + bias, inverse)


def middle_kernel(spots, *refs):
    sizes, gathered_ref, conv_ref, *cot_refs = refs[0:7]
    gain_ref, bias_ref, slope_ref, moments_ref, payload_ref, packed = refs[7:13]
    channels = gain_ref.shape[1]
    parts = channels // 128
    block = 4 * parts
    sums = gathered_ref[:, 0:block, :]
    spreads = gathered_ref[:, block : 2 * block, :]
    counts = gathered_ref[:, 2 * block : 3 * block, :]
    total_count = jnp.sum(counts, axis=0)
    mean_rows = jnp.sum(sums, axis=0) / total_count
    offset = sums / counts - mean_rows[None]
    variance = jnp.sum(spreads + counts * offset * offset, axis=0) / total_count
    moments_ref[0:block, :] = mean_rows
    moments_ref[block : 2 * block, :] = lax.rsqrt(variance + EPSILON)
    moments_ref[2 * block : 3 * block, :] = total_count
    for level_index, (cot_ref, (row, column, extent)) in enumerate(zip(cot_refs, spots)):
        limits = level_limits(sizes, level_index, extent)
        normed, shifted, inverse = normalized(spots, level_index, conv_ref, moments_ref, gain_ref, bias_ref)
        sigmoid_value = 1.0 / (1.0 + jnp.exp(-shifted))
        slope = cot_ref[0].astype(jnp.float32) * sigmoid_value * (1.0 + shifted * (1.0 - sigmoid_value))
        slope = jnp.where(inside_mask(limits, slope.shape), slope, 0.0)
        slope_ref[row - 1 : row - 1 + extent, column : column + extent, :] = slope
        put_row(packed, level_index * parts, jnp.sum(slope, axis=(0, 1)).reshape(1, channels))
        put_row(packed, (4 + level_index) * parts, jnp.sum(slope * normed, axis=(0, 1)).reshape(1, channels))
    payload_ref[...] = jnp.broadcast_to(packed[...][None], payload_ref.shape)


def weight_grad_rows(spread_ref, back_ref, first, target_ref):
    cells, channels = back_ref.shape
    body = cells - 2 * PITCH
    step = channels // 2
    turned = back_ref[PITCH : PITCH + body, :]
    for start in range(0, target_ref.shape[0], step):
        place = first + start
        tap_row = lax.div(place, 3 * channels)
        lane = pl.multiple_of(place - tap_row * 3 * channels, 128)
        window = spread_ref[pl.ds(pl.multiple_of(tap_row * PITCH, PITCH), body), pl.ds(lane, step)]
        target_ref[start : start + step, :] = lax.dot_general(
            window, turned, (((0,), (0,)), ((), ())), preferred_element_type=jnp.float32
        )


def back_kernel(spots, devices, *refs):
    sizes, gathered_ref, conv_ref, slope_ref, moments_ref, gain_ref, bias_ref, spread_ref = refs[0:8]
    back_ref, send_ref, d_gain_ref, d_shift_ref, wide_back = refs[8:13]
    channels = gain_ref.shape[1]
    parts = channels // 128
    block = 4 * parts
    shift_rows = jnp.sum(gathered_ref[:, 0:block, :], axis=0)
    gain_rows = jnp.sum(gathered_ref[:, block : 2 * block, :], axis=0)
    wide_back[...] = jnp.zeros_like(wide_back)
    for level_index, (row, column, extent) in enumerate(spots):
        limits = level_limits(sizes, level_index, extent)
        normed, shifted, inverse = normalized(spots, level_index, conv_ref, moments_ref, gain_ref, bias_ref)
        count = get_row(moments_ref[2 * block : 3 * block, :], level_index, parts)[None]
        shift_sum = get_row(shift_rows, level_index, parts)
        gain_sum = get_row(gain_rows, level_index, parts)
        d_gain_ref[level_index : level_index + 1, :] = gain_sum / devices
        d_shift_ref[level_index : level_index + 1, :] = shift_sum / devices
        gain = gain_ref[level_index : level_index + 1, :][None]
        slope = slope_ref[row - 1 : row - 1 + extent, column : column + extent, :]
        back = (gain * inverse) * (slope - shift_sum[None] / count - normed * (gain_sum[None] / count))
        back = jnp.where(inside_mask(limits, back.shape), back, 0.0)
        wide_back[row : row + extent, column : column + extent, :] = back
    rows = wide_back.shape[0]
    back_ref[...] = wide_back[...].reshape(rows * PITCH, channels).astype(jnp.bfloat16)
    half = send_ref.shape[0]
    core_size = (9 * channels) // half
    first = (core_size - 1 - places()[0]) * half
    weight_grad_rows(spread_ref, back_ref, first, send_ref)


def tail_kernel(spots, *refs):
    sizes, back_ref, spread_ref, conv_ref, moments_ref, gain_ref, bias_ref, keep_ref, *out_refs = refs
    half = keep_ref.shape[0]
    weight_grad_rows(spread_ref, back_ref, places()[0] * half, keep_ref)
    for level_index, (out_ref, (row, column, extent)) in enumerate(zip(out_refs, spots)):
        limits = level_limits(sizes, level_index, extent)
        normed, shifted, inverse = normalized(spots, level_index, conv_ref, moments_ref, gain_ref, bias_ref)
        values = shifted * (1.0 / (1.0 + jnp.exp(-shifted)))
        out_ref[0] = jnp.where(inside_mask(limits, values.shape), values, 0.0).astype(jnp.bfloat16)


def input_grad_kernel(spots, sizes, back_ref, weight_ref, *refs):
    *target_refs, spread, summed = refs
    cells, channels = back_ref.shape
    rows = cells // PITCH
    body = (rows - 2) * PITCH
    spread_columns(back_ref[...].astype(jnp.float32), spread)
    total = jnp.zeros((body, channels), jnp.float32)
    for tap_row in range(3):
        for tap_col in range(3):
            start = (2 - tap_row) * PITCH
            lane = (2 - tap_col) * channels
            total = total + lax.dot_general(
                spread[start : start + body, lane : lane + channels],
                weight_ref[tap_row, tap_col * channels : (tap_col + 1) * channels, :],
                (((1,), (1,)), ((), ())),
                preferred_element_type=jnp.float32,
            )
    summed[...] = total.reshape(rows - 2, PITCH, channels)
    for level_index, (target_ref, (row, column, extent)) in enumerate(zip(target_refs, spots)):
        limits = level_limits(sizes, level_index, extent)
        values = summed[row - 1 : row - 1 + extent, column : column + extent, :]
        target_ref[0] = jnp.where(inside_mask(limits, values.shape), values, 0.0).astype(jnp.bfloat16)


def stage_place(stage):
    return places()[stage]


def add_and_cut_kernel(stage, size, count, *refs):
    parts, pieces = refs[:count], refs[count:]
    rows = pieces[0].shape[0]
    place = stage_place(stage)
    for step, piece_ref in enumerate(pieces):
        start = pl.multiple_of(lax.rem(place + step, size) * rows, 8)
        total = parts[0][pl.ds(start, rows), :]
        for part in parts[1:]:
            total = total + part[pl.ds(start, rows), :]
        piece_ref[...] = total


def add_and_scale_kernel(scale, *refs):
    total = refs[0][...]
    for part in refs[1:-1]:
        total = total + part[...]
    refs[-1][...] = total * scale


def join_kernel(stage, size, *refs):
    pieces, whole_ref = refs[:size], refs[size]
    rows = pieces[0].shape[0]
    place = stage_place(stage)
    for step, piece_ref in enumerate(pieces):
        start = pl.multiple_of(lax.rem(place - step + size, size) * rows, 8)
        whole_ref[pl.ds(start, rows), :] = piece_ref[...]


def call(kernel, name, outputs, in_specs, scratch=(), flops=0, out_specs=None):
    return pl.pallas_call(
        kernel,
        out_shape=outputs,
        in_specs=in_specs,
        out_specs=jax.tree.map(lambda leaf: VMEM, outputs) if out_specs is None else out_specs,
        scratch_shapes=scratch,
        compiler_params=pltpu.CompilerParams(vmem_limit_bytes=20 * 1024 * 1024),
        cost_estimate=pl.CostEstimate(flops=flops, bytes_accessed=0, transcendentals=0),
        name=name,
    )


def layout():
    group_size = lax.axis_size("group")
    wide_size = lax.axis_size("wide")
    core_size = 2 if group_size % 2 == 0 else 1
    col_size = group_size // core_size
    row_size = col_size if wide_size % col_size == 0 else 1
    return (core_size, col_size, row_size, wide_size // row_size)


def places():
    core_size, col_size, row_size, deep_size = layout()
    group_index = lax.axis_index("group")
    wide_index = lax.axis_index("wide")
    core = lax.rem(group_index, core_size)
    plane = lax.rem(wide_index, row_size) * col_size + lax.div(group_index, core_size)
    return (core, plane, lax.div(wide_index, row_size))


def exchange(values, core_step, plane_step, deep_step):
    core_size, col_size, row_size, deep_size = layout()
    plane_size = col_size * row_size
    pairs = []
    for deep in range(deep_size):
        for plane in range(plane_size):
            for core in range(core_size):
                ends = []
                for core_end, plane_end, deep_end in (
                    (core, plane, deep),
                    (
                        (core + core_step) % core_size,
                        (plane + plane_step) % plane_size,
                        (deep + deep_step) % deep_size,
                    ),
                ):
                    wide_index = deep_end * row_size + plane_end // col_size
                    group_index = (plane_end % col_size) * core_size + core_end
                    ends.append(wide_index * col_size * core_size + group_index)
                pairs.append(tuple(ends))
    return lax.ppermute(values, ("wide", "group"), pairs)


def scatter_stage(parts, stage, size, send):
    rows, lanes = parts[0].shape
    piece_rows = rows // size
    if piece_rows % 8:
        total = sum(parts[1:], parts[0])
        pieces = [
            lax.dynamic_slice_in_dim(total, ((places()[stage] + step) % size) * piece_rows, piece_rows, 0)
            for step in range(size)
        ]
    else:
        pieces = call(
            partial(add_and_cut_kernel, stage, size, len(parts)),
            "add_and_cut",
            (struct((piece_rows, lanes)),) * size,
            [VMEM] * len(parts),
            flops=rows * lanes,
        )(*parts)
    return [pieces[0]] + [send(pieces[step], step) for step in range(1, size)]


def join_stage(pieces, stage, target=None):
    rows, lanes = pieces[0].shape
    size = len(pieces)
    if rows % 8:
        whole = jnp.zeros((rows * size, lanes), pieces[0].dtype)
        for step, part in enumerate(pieces):
            start = ((places()[stage] - step) % size) * rows
            whole = lax.dynamic_update_slice_in_dim(whole, part, start, 0)
        return whole
    return call(
        partial(join_kernel, stage, size),
        "join",
        struct((rows * size, lanes)),
        [VMEM] * size,
        flops=rows * size * lanes,
    )(*pieces)


def gather_stage(values, stage, size, send):
    return join_stage([values] + [send(values, step) for step in range(1, size)], stage)


def swap_stats(payload):
    return lax.all_to_all(payload, ("wide", "group"), 0, 0)


def combine_grads(keep, send, devices):
    core_size, col_size, row_size, deep_size = layout()
    plane_size = col_size * row_size
    send_core = lambda part, step: exchange(part, step, 0, 0)
    send_plane = lambda part, step: exchange(part, 0, step, 0)
    send_deep = lambda part, step: exchange(part, 0, 0, step)
    parts = [keep]
    if core_size > 1:
        parts.append(send_core(send, 1))
    parts = scatter_stage(parts, 1, plane_size, send_plane)
    parts = scatter_stage(parts, 2, deep_size, send_deep)
    own = call(
        partial(add_and_scale_kernel, 1.0 / devices),
        "add_and_scale",
        struct(parts[0].shape),
        [VMEM] * len(parts),
    )(*parts)
    own = gather_stage(own, 2, deep_size, send_deep)
    own = gather_stage(own, 1, plane_size, send_plane)
    return gather_stage(own, 0, core_size, send_core)


def in_hbm(leaf):
    return pltpu.with_memory_space_constraint(leaf, pltpu.HBM)


def struct(shape, dtype=jnp.float32):
    return jax.ShapeDtypeStruct(shape, dtype)


def shards(
    feat4,
    feat5,
    feat6,
    feat7,
    out_grad4,
    out_grad5,
    out_grad6,
    out_grad7,
    conv_weight,
    bn_gain,
    bn_shift,
    heights,
    widths,
):
    features = (feat4, feat5, feat6, feat7)
    cotangents = (out_grad4, out_grad5, out_grad6, out_grad7)
    devices = lax.axis_size("wide") * lax.axis_size("group")
    core_size = layout()[0]
    channels = conv_weight.shape[2]
    parts = channels // 128
    spots, rows = canvas_spots(tuple(feature.shape[1] for feature in features))
    cells = rows * PITCH
    body = cells - 2 * PITCH
    folded = conv_weight.reshape(3, 3 * channels, channels)
    work = 2 * body * 9 * channels * channels
    half = 9 * channels // core_size
    levels = tuple(struct(feature.shape, jnp.bfloat16) for feature in features)
    canvas = pltpu.VMEM((rows, PITCH, channels), jnp.float32)

    sizes = jnp.concatenate([heights, widths]).reshape(2, 1)
    spread, conv_out, payload = call(
        partial(forward_kernel, spots, rows),
        "forward",
        (
            struct((cells, 3 * channels), jnp.bfloat16),
            struct((rows - 2, PITCH, channels)),
            struct((devices, 12 * parts, 128)),
        ),
        [VMEM] + [HBM] * 5,
        [canvas, pltpu.VMEM((12 * parts, 128), jnp.float32), pltpu.VMEM(folded.shape, folded.dtype)]
        + [pltpu.VMEM(feature.shape, feature.dtype) for feature in features]
        + [pltpu.SemaphoreType.DMA((5,))],
        flops=work,
    )(sizes, *(in_hbm(leaf) for leaf in (*features, folded)))
    gathered = swap_stats(payload)
    slope, moments, payload = call(
        partial(middle_kernel, spots),
        "middle",
        (
            struct((rows - 2, PITCH, channels)),
            struct((12 * parts, 128)),
            struct((devices, 8 * parts, 128)),
        ),
        [VMEM] * 9,
        [pltpu.VMEM((8 * parts, 128), jnp.float32)],
        flops=body * channels * 100,
    )(sizes, gathered, conv_out, *cotangents, bn_gain, bn_shift)
    gathered = swap_stats(payload)
    back, send, d_gain, d_shift = call(
        partial(back_kernel, spots, devices),
        "back",
        (
            struct((cells, channels), jnp.bfloat16),
            struct((half, channels)),
            struct(bn_gain.shape),
            struct(bn_gain.shape),
        ),
        [VMEM] * 8,
        [canvas],
        flops=work // core_size,
    )(sizes, gathered, conv_out, slope, moments, bn_gain, bn_shift, spread)
    keep, *outputs = call(
        partial(tail_kernel, spots),
        "tail",
        (struct((half, channels)),) + levels,
        [VMEM] * 7,
        flops=work // core_size,
    )(sizes, back, spread, conv_out, moments, bn_gain, bn_shift)
    input_grads = call(
        partial(input_grad_kernel, spots),
        "input_grad",
        levels,
        [VMEM] * 3,
        [
            pltpu.VMEM((cells, 3 * channels), jnp.bfloat16),
            pltpu.VMEM((rows - 2, PITCH, channels), jnp.float32),
        ],
        flops=work,
    )(sizes, back, folded)
    weight_total = combine_grads(keep, send, devices).reshape(conv_weight.shape)
    return (*outputs, *input_grads, weight_total, d_gain, d_shift)


def solution(mesh):
    placed = (
        P(("wide", "group"), None, None, None),
        P(("wide", "group"), None, None, None),
        P(("wide", "group"), None, None, None),
        P(("wide", "group"), None, None, None),
        P(("wide", "group"), None, None, None),
        P(("wide", "group"), None, None, None),
        P(("wide", "group"), None, None, None),
        P(("wide", "group"), None, None, None),
        P(),
        P(),
        P(),
        P(("wide", "group")),
        P(("wide", "group")),
    )
    return jax.shard_map(
        shards,
        mesh=mesh,
        in_specs=placed,
        out_specs=(
            P(("wide", "group"), None, None, None),
            P(("wide", "group"), None, None, None),
            P(("wide", "group"), None, None, None),
            P(("wide", "group"), None, None, None),
            P(("wide", "group"), None, None, None),
            P(("wide", "group"), None, None, None),
            P(("wide", "group"), None, None, None),
            P(("wide", "group"), None, None, None),
            P(),
            P(),
            P(),
        ),
        check_vma=False,
    )
```

```python
from functools import partial

import jax
import jax.numpy as jnp
from jax import lax
from jax.experimental import pallas as pl
from jax.experimental.pallas import tpu as pltpu
from jax.sharding import PartitionSpec as P

EPSILON = 1e-05
PITCH = 32
STRIDE = 16
VMEM = pl.BlockSpec(memory_space=pltpu.VMEM)
HBM = pl.BlockSpec(memory_space=pltpu.HBM)


def canvas_spots(extents):
    spots = [(1, 0, extents[0])]
    column = 0
    for extent in extents[1:]:
        spots.append((extents[0] + 2, column, extent))
        column += -(-(extent + 1) // 8) * 8
    rows = extents[0] + extents[1] + 3
    assert column <= PITCH and extents[0] < PITCH
    return tuple(spots), rows


def level_limits(sizes_ref, level_index, extent):
    stride = STRIDE * 2**level_index
    shift = stride.bit_length() - 1
    limits = []
    for line in range(2):
        pixels = sizes_ref[line : line + 1, 0:1].reshape(1, 1, 1)
        limits.append(jnp.minimum(lax.shift_right_arithmetic(pixels + (stride - 1), shift), extent))
    return tuple(limits)


def inside_mask(limits, shape):
    row_place = lax.broadcasted_iota(jnp.int32, shape, 0)
    col_place = lax.broadcasted_iota(jnp.int32, shape, 1)
    return jnp.logical_and(row_place < limits[0], col_place < limits[1])


def put_row(ref, row, vector):
    for part in range(vector.shape[1] // 128):
        ref[row + part : row + part + 1, :] = vector[:, part * 128 : (part + 1) * 128]


def get_row(packed, level_index, parts):
    rows = [packed[level_index * parts + part : level_index * parts + part + 1, :] for part in range(parts)]
    return jnp.concatenate(rows, axis=1)


def spread_columns(flat, target):
    cells, channels = flat.shape
    target[:, 0:channels] = pltpu.roll(flat, 1, 0).astype(jnp.bfloat16)
    target[:, channels : 2 * channels] = flat.astype(jnp.bfloat16)
    target[:, 2 * channels :] = pltpu.roll(flat, cells - 1, 0).astype(jnp.bfloat16)


def forward_kernel(spots, rows, *refs):
    sizes, *features_in = refs[0:5]
    weight_in, spread_ref, conv_ref, payload_ref, canvas, packed, weight_ref, *feature_refs = refs[5:16]
    semaphores = refs[16]
    copies = [
        pltpu.make_async_copy(source, target, semaphores.at[place])
        for place, (source, target) in enumerate(
            zip(
                (*features_in, weight_in),
                (*feature_refs, weight_ref),
            )
        )
    ]
    for copy in copies:
        copy.start()
    channels = weight_ref.shape[2]
    parts = channels // 128
    canvas[...] = jnp.zeros_like(canvas)
    packed[:, 8 * channels :] = jnp.zeros((1, 128), jnp.float32)
    for copy in copies[:-1]:
        copy.wait()
    for level_index, (feat_ref, (row, column, extent)) in enumerate(zip(feature_refs, spots)):
        limits = level_limits(sizes, level_index, extent)
        values = feat_ref[0].astype(jnp.float32)
        inside = inside_mask(limits, values.shape)
        canvas[row : row + extent, column : column + extent, :] = jnp.where(inside, values, 0.0)
    spread_columns(canvas[...].reshape(rows * PITCH, channels), spread_ref)
    body = (rows - 2) * PITCH
    copies[-1].wait()
    summed = jnp.zeros((body, channels), jnp.float32)
    for tap_row in range(3):
        summed = summed + jnp.dot(
            spread_ref[tap_row * PITCH : tap_row * PITCH + body, :],
            weight_ref[tap_row],
            preferred_element_type=jnp.float32,
        )
    conv_ref[...] = summed.reshape(rows - 2, PITCH, channels)
    for level_index, (row, column, extent) in enumerate(spots):
        limits = level_limits(sizes, level_index, extent)
        conv_out = conv_ref[row - 1 : row - 1 + extent, column : column + extent, :]
        inside = inside_mask(limits, conv_out.shape)
        count = (limits[0] * limits[1]).astype(jnp.float32).reshape(1, 1)
        total = jnp.sum(jnp.where(inside, conv_out, 0.0), axis=(0, 1)).reshape(1, channels)
        centered = jnp.where(inside, conv_out - total / count, 0.0)
        spread = jnp.sum(centered * centered, axis=(0, 1)).reshape(1, channels)
        packed[:, level_index * channels : (level_index + 1) * channels] = total
        packed[:, (4 + level_index) * channels : (5 + level_index) * channels] = spread
        packed[:, 8 * channels + level_index : 8 * channels + level_index + 1] = count
    payload_ref[...] = jnp.broadcast_to(packed[...][None], payload_ref.shape)


def normalized(spots, level_index, conv_ref, moments_ref, gain_ref, bias_ref):
    row, column, extent = spots[level_index]
    mean_value = moments_ref[level_index : level_index + 1, :][None]
    inverse = moments_ref[4 + level_index : 5 + level_index, :][None]
    gain = gain_ref[level_index : level_index + 1, :][None]
    bias = bias_ref[level_index : level_index + 1, :][None]
    conv_out = conv_ref[row - 1 : row - 1 + extent, column : column + extent, :]
    normed = (conv_out - mean_value) * inverse
    return (normed, gain * normed + bias, inverse)


def middle_kernel(spots, *refs):
    sizes, gathered_ref, conv_ref, *cot_refs = refs[0:7]
    gain_ref, bias_ref, slope_ref, moments_ref, payload_ref, packed = refs[7:13]
    channels = gain_ref.shape[1]
    parts = channels // 128
    for level_index in range(4):
        sums = gathered_ref[:, :, level_index * channels : (level_index + 1) * channels]
        spreads = gathered_ref[:, :, (4 + level_index) * channels : (5 + level_index) * channels]
        counts = gathered_ref[:, :, 8 * channels + level_index : 8 * channels + level_index + 1]
        total_count = jnp.sum(counts, axis=0)
        mean_value = jnp.sum(sums, axis=0) / total_count
        offset = sums * (1.0 / counts) - mean_value[None]
        variance = jnp.sum(spreads + counts * offset * offset, axis=0) / total_count
        moments_ref[level_index : level_index + 1, :] = mean_value
        moments_ref[4 + level_index : 5 + level_index, :] = lax.rsqrt(variance + EPSILON)
        moments_ref[8 + level_index : 9 + level_index, :] = jnp.broadcast_to(total_count, (1, channels))
    for level_index, (cot_ref, (row, column, extent)) in enumerate(zip(cot_refs, spots)):
        limits = level_limits(sizes, level_index, extent)
        normed, shifted, inverse = normalized(spots, level_index, conv_ref, moments_ref, gain_ref, bias_ref)
        sigmoid_value = 1.0 / (1.0 + jnp.exp(-shifted))
        slope = cot_ref[0].astype(jnp.float32) * sigmoid_value * (1.0 + shifted * (1.0 - sigmoid_value))
        slope = jnp.where(inside_mask(limits, slope.shape), slope, 0.0)
        slope_ref[row - 1 : row - 1 + extent, column : column + extent, :] = slope
        put_row(packed, level_index * parts, jnp.sum(slope, axis=(0, 1)).reshape(1, channels))
        put_row(packed, (4 + level_index) * parts, jnp.sum(slope * normed, axis=(0, 1)).reshape(1, channels))
    payload_ref[...] = jnp.broadcast_to(packed[...][None], payload_ref.shape)


def weight_grad_rows(spread_ref, back_ref, first, target_ref):
    cells, channels = back_ref.shape
    body = cells - 2 * PITCH
    step = channels // 2
    turned = back_ref[PITCH : PITCH + body, :]
    for start in range(0, target_ref.shape[0], step):
        place = first + start
        tap_row = lax.div(place, 3 * channels)
        lane = pl.multiple_of(place - tap_row * 3 * channels, 128)
        window = spread_ref[pl.ds(pl.multiple_of(tap_row * PITCH, PITCH), body), pl.ds(lane, step)]
        target_ref[start : start + step, :] = lax.dot_general(
            window, turned, (((0,), (0,)), ((), ())), preferred_element_type=jnp.float32
        )


def back_kernel(spots, devices, *refs):
    sizes, gathered_ref, conv_ref, slope_ref, moments_ref, gain_ref, bias_ref, spread_ref = refs[0:8]
    back_ref, send_ref, d_gain_ref, d_shift_ref, wide_back = refs[8:13]
    channels = gain_ref.shape[1]
    parts = channels // 128
    block = 4 * parts
    shift_rows = jnp.sum(gathered_ref[:, 0:block, :], axis=0)
    gain_rows = jnp.sum(gathered_ref[:, block : 2 * block, :], axis=0)
    wide_back[...] = jnp.zeros_like(wide_back)
    for level_index, (row, column, extent) in enumerate(spots):
        limits = level_limits(sizes, level_index, extent)
        normed, shifted, inverse = normalized(spots, level_index, conv_ref, moments_ref, gain_ref, bias_ref)
        count = moments_ref[8 + level_index : 9 + level_index, :][None]
        shift_sum = get_row(shift_rows, level_index, parts)
        gain_sum = get_row(gain_rows, level_index, parts)
        d_gain_ref[level_index : level_index + 1, :] = gain_sum / devices
        d_shift_ref[level_index : level_index + 1, :] = shift_sum / devices
        gain = gain_ref[level_index : level_index + 1, :][None]
        slope = slope_ref[row - 1 : row - 1 + extent, column : column + extent, :]
        back = (gain * inverse) * (slope - shift_sum[None] / count - normed * (gain_sum[None] / count))
        back = jnp.where(inside_mask(limits, back.shape), back, 0.0)
        wide_back[row : row + extent, column : column + extent, :] = back
    rows = wide_back.shape[0]
    back_ref[...] = wide_back[...].reshape(rows * PITCH, channels).astype(jnp.bfloat16)
    half = send_ref.shape[0]
    core_size = (9 * channels) // half
    first = (core_size - 1 - places()[0]) * half
    weight_grad_rows(spread_ref, back_ref, first, send_ref)


def keep_kernel(back_ref, spread_ref, keep_ref):
    weight_grad_rows(spread_ref, back_ref, places()[0] * keep_ref.shape[0], keep_ref)


def output_kernel(spots, sizes, conv_ref, moments_ref, gain_ref, bias_ref, *out_refs):
    for level_index, (out_ref, (row, column, extent)) in enumerate(zip(out_refs, spots)):
        limits = level_limits(sizes, level_index, extent)
        normed, shifted, inverse = normalized(spots, level_index, conv_ref, moments_ref, gain_ref, bias_ref)
        values = shifted * (1.0 / (1.0 + jnp.exp(-shifted)))
        out_ref[0] = jnp.where(inside_mask(limits, values.shape), values, 0.0).astype(jnp.bfloat16)


def input_grad_kernel(spots, sizes, back_ref, weight_ref, *refs):
    *target_refs, spread, summed = refs
    cells, channels = back_ref.shape
    rows = cells // PITCH
    body = (rows - 2) * PITCH
    spread_columns(back_ref[...].astype(jnp.float32), spread)
    total = jnp.zeros((body, channels), jnp.float32)
    for tap_row in range(3):
        for tap_col in range(3):
            start = (2 - tap_row) * PITCH
            lane = (2 - tap_col) * channels
            total = total + lax.dot_general(
                spread[start : start + body, lane : lane + channels],
                weight_ref[tap_row, tap_col * channels : (tap_col + 1) * channels, :],
                (((1,), (1,)), ((), ())),
                preferred_element_type=jnp.float32,
            )
    summed[...] = total.reshape(rows - 2, PITCH, channels)
    for level_index, (target_ref, (row, column, extent)) in enumerate(zip(target_refs, spots)):
        limits = level_limits(sizes, level_index, extent)
        values = summed[row - 1 : row - 1 + extent, column : column + extent, :]
        target_ref[0] = jnp.where(inside_mask(limits, values.shape), values, 0.0).astype(jnp.bfloat16)


def stage_place(stage):
    return places()[stage]


def add_and_cut_kernel(stage, size, count, *refs):
    parts, pieces = refs[:count], refs[count:]
    rows = pieces[0].shape[0]
    place = stage_place(stage)
    for step, piece_ref in enumerate(pieces):
        start = pl.multiple_of(partner(place, step, size) * rows, 8)
        total = parts[0][pl.ds(start, rows), :]
        for part in parts[1:]:
            total = total + part[pl.ds(start, rows), :]
        piece_ref[...] = total


def add_and_scale_kernel(scale, *refs):
    total = refs[0][...]
    for part in refs[1:-1]:
        total = total + part[...]
    refs[-1][...] = total * scale


def join_kernel(stage, size, *refs):
    pieces, whole_ref = refs[:size], refs[size]
    rows = pieces[0].shape[0]
    place = stage_place(stage)
    for step, piece_ref in enumerate(pieces):
        start = pl.multiple_of(origin(place, step, size) * rows, 8)
        whole_ref[pl.ds(start, rows), :] = piece_ref[...]


def cut_kernel(plane_size, deep_size, count, *refs):
    parts, pieces = refs[:count], refs[count:]
    rows = pieces[1].shape[0]
    core, plane, deep = places()
    for step in range(plane_size):
        away_ref, own_ref = pieces[2 * step : 2 * step + 2]
        base = partner(plane, step, plane_size) * (rows * deep_size)
        for deep_step in range(deep_size):
            start = pl.multiple_of(base + partner(deep, deep_step, deep_size) * rows, 8)
            total = parts[0][pl.ds(start, rows), :]
            for part in parts[1:]:
                total = total + part[pl.ds(start, rows), :]
            if deep_step == 0:
                own_ref[...] = total
            else:
                away_ref[(deep_step - 1) * rows : deep_step * rows, :] = total


def add_split_kernel(count, *refs):
    parts, pieces = refs[:count], refs[count:]
    rows = pieces[0].shape[0]
    for place, piece_ref in enumerate(pieces):
        total = parts[0][place * rows : (place + 1) * rows, :]
        for part in parts[1:]:
            total = total + part[place * rows : (place + 1) * rows, :]
        piece_ref[...] = total


def lay_kernel(plane_size, core_step, *refs):
    pieces = refs[-(plane_size + 2) : -2]
    whole_ref, semaphore = refs[-2:]
    rows = pieces[0].shape[0]
    core, plane, deep = places()
    first = origin(core, core_step, layout()[0]) * (rows * plane_size)
    copies = []
    for step, piece_ref in enumerate(pieces):
        start = pl.multiple_of(first + origin(plane, step, plane_size) * rows, 8)
        target = whole_ref.at[pl.ds(start, rows), :]
        copies.append(pltpu.make_async_copy(piece_ref, target, semaphore.at[step]))
    for copy in copies:
        copy.start()
    for copy in copies:
        copy.wait()


def call(kernel, name, outputs, in_specs, scratch=(), flops=0, out_specs=None, aliases=None):
    return pl.pallas_call(
        input_output_aliases=aliases or {},
        kernel=kernel,
        out_shape=outputs,
        in_specs=in_specs,
        out_specs=jax.tree.map(lambda leaf: VMEM, outputs) if out_specs is None else out_specs,
        scratch_shapes=scratch,
        compiler_params=pltpu.CompilerParams(vmem_limit_bytes=20 * 1024 * 1024),
        cost_estimate=pl.CostEstimate(flops=flops, bytes_accessed=0, transcendentals=0),
        name=name,
    )


def layout():
    group_size = lax.axis_size("group")
    wide_size = lax.axis_size("wide")
    core_size = 2 if group_size % 2 == 0 else 1
    col_size = group_size // core_size
    row_size = col_size if wide_size % col_size == 0 else 1
    return (core_size, col_size, row_size, wide_size // row_size)


def places():
    core_size, col_size, row_size, deep_size = layout()
    group_index = lax.axis_index("group")
    wide_index = lax.axis_index("wide")
    core = lax.rem(group_index, core_size)
    plane = lax.rem(wide_index, row_size) * col_size + lax.div(group_index, core_size)
    return (core, plane, lax.div(wide_index, row_size))


def partner(place, step, size):
    if size & (size - 1) == 0:
        return place ^ step
    return lax.rem(place + step, size) if isinstance(place, jax.Array) else (place + step) % size


def origin(place, step, size):
    return partner(place, step if size & (size - 1) == 0 else size - step, size)


def exchange(values, core_step, plane_step, deep_step):
    core_size, col_size, row_size, deep_size = layout()
    plane_size = col_size * row_size
    pairs = []
    for deep in range(deep_size):
        for plane in range(plane_size):
            for core in range(core_size):
                ends = []
                for core_end, plane_end, deep_end in (
                    (core, plane, deep),
                    (
                        partner(core, core_step, core_size),
                        partner(plane, plane_step, plane_size),
                        partner(deep, deep_step, deep_size),
                    ),
                ):
                    wide_index = deep_end * row_size + plane_end // col_size
                    group_index = (plane_end % col_size) * core_size + core_end
                    ends.append(wide_index * col_size * core_size + group_index)
                pairs.append(tuple(ends))
    return lax.ppermute(values, ("wide", "group"), pairs)


def scatter_stage(parts, stage, size, send):
    rows, lanes = parts[0].shape
    piece_rows = rows // size
    if piece_rows % 8:
        total = sum(parts[1:], parts[0])
        pieces = [
            lax.dynamic_slice_in_dim(total, partner(places()[stage], step, size) * piece_rows, piece_rows, 0)
            for step in range(size)
        ]
    else:
        pieces = call(
            partial(add_and_cut_kernel, stage, size, len(parts)),
            "add_and_cut",
            (struct((piece_rows, lanes)),) * size,
            [VMEM] * len(parts),
            flops=rows * lanes,
        )(*parts)
    return [pieces[0]] + [send(pieces[step], step) for step in range(1, size)]


def join_stage(pieces, stage, target=None):
    rows, lanes = pieces[0].shape
    size = len(pieces)
    if rows % 8:
        whole = jnp.zeros((rows * size, lanes), pieces[0].dtype)
        for step, part in enumerate(pieces):
            start = origin(places()[stage], step, size) * rows
            whole = lax.dynamic_update_slice_in_dim(whole, part, start, 0)
        return whole
    return call(
        partial(join_kernel, stage, size),
        "join",
        struct((rows * size, lanes)),
        [VMEM] * size,
        flops=rows * size * lanes,
    )(*pieces)


def gather_stage(values, stage, size, send):
    return join_stage([values] + [send(values, step) for step in range(1, size)], stage)


def swap_stats(payload):
    return lax.all_to_all(payload, ("wide", "group"), 0, 0)


def send_core(part, step):
    return exchange(part, step, 0, 0)


def send_plane(part, step):
    return exchange(part, 0, step, 0)


def send_deep(part, step):
    return exchange(part, 0, 0, step)


def scatter_grads(keep, send, beside):
    core_size, col_size, row_size, deep_size = layout()
    plane_size = col_size * row_size
    parts = [keep]
    if core_size > 1:
        parts.append(send_core(send, 1))
    rows, lanes = keep.shape
    rows //= plane_size * deep_size
    if rows % 8 or deep_size == 1:
        parts = scatter_stage(parts, 1, plane_size, send_plane)
        return (scatter_stage(parts, 2, deep_size, send_deep), beside)
    shapes = (struct(((deep_size - 1) * rows, lanes)), struct((rows, lanes))) * plane_size
    pieces = call(
        partial(cut_kernel, plane_size, deep_size, len(parts)), "cut", shapes, [VMEM] * len(parts), flops=keep.size
    )(*parts)
    away = [pieces[0]] + [send_plane(pieces[2 * step], step) for step in range(1, plane_size)]
    own = [pieces[1]] + [send_plane(pieces[2 * step + 1], step) for step in range(1, plane_size)]
    pieces = call(
        partial(add_split_kernel, plane_size),
        "add_split",
        (struct((rows, lanes)),) * (deep_size - 1),
        [VMEM] * plane_size,
        flops=keep.size,
    )(*away)
    pieces, beside = lax.optimization_barrier((pieces, beside))
    return (own + [send_deep(piece, step + 1) for step, piece in enumerate(pieces)], beside)


def gather_grads(own):
    core_size, col_size, row_size, deep_size = layout()
    plane_size = col_size * row_size
    rows, lanes = own.shape
    half = rows * plane_size * deep_size
    if rows % 8 or deep_size == 1:
        own = gather_stage(own, 2, deep_size, send_deep)
        own = gather_stage(own, 1, plane_size, send_plane)
        return gather_stage(own, 0, core_size, send_core)
    own = gather_stage(own, 2, deep_size, send_deep)
    pieces = [own] + [send_plane(own, step) for step in range(1, plane_size)]
    shape = struct((half * core_size, lanes))
    scratch = [pltpu.SemaphoreType.DMA((plane_size,))]
    total = call(
        partial(lay_kernel, plane_size, 0), "lay", shape, [VMEM] * plane_size, scratch, half * lanes, HBM
    )(*pieces)
    for core_step in range(1, core_size):
        others = [send_core(piece, core_step) for piece in pieces]
        total = call(
            partial(lay_kernel, plane_size, core_step),
            "lay_other",
            shape,
            [HBM] + [VMEM] * plane_size,
            scratch,
            half * lanes,
            HBM,
            {0: 0},
        )(total, *others)
    return total


def in_hbm(leaf):
    return pltpu.with_memory_space_constraint(leaf, pltpu.HBM)


def struct(shape, dtype=jnp.float32):
    return jax.ShapeDtypeStruct(shape, dtype)


def shards(
    feat4,
    feat5,
    feat6,
    feat7,
    out_grad4,
    out_grad5,
    out_grad6,
    out_grad7,
    conv_weight,
    bn_gain,
    bn_shift,
    heights,
    widths,
):
    features = (feat4, feat5, feat6, feat7)
    cotangents = (out_grad4, out_grad5, out_grad6, out_grad7)
    devices = lax.axis_size("wide") * lax.axis_size("group")
    core_size = layout()[0]
    channels = conv_weight.shape[2]
    parts = channels // 128
    spots, rows = canvas_spots(tuple(feature.shape[1] for feature in features))
    cells = rows * PITCH
    body = cells - 2 * PITCH
    folded = conv_weight.reshape(3, 3 * channels, channels)
    work = 2 * body * 9 * channels * channels
    half = 9 * channels // core_size
    levels = tuple(struct(feature.shape, jnp.bfloat16) for feature in features)
    canvas = pltpu.VMEM((rows, PITCH, channels), jnp.float32)

    sizes = jnp.concatenate([heights, widths]).reshape(2, 1)
    spread, conv_out, payload = call(
        partial(forward_kernel, spots, rows),
        "forward",
        (
            struct((cells, 3 * channels), jnp.bfloat16),
            struct((rows - 2, PITCH, channels)),
            struct((devices, 1, 8 * channels + 128)),
        ),
        [VMEM] + [HBM] * 5,
        [canvas, pltpu.VMEM((1, 8 * channels + 128), jnp.float32), pltpu.VMEM(folded.shape, folded.dtype)]
        + [pltpu.VMEM(feature.shape, feature.dtype) for feature in features]
        + [pltpu.SemaphoreType.DMA((5,))],
        flops=work,
    )(sizes, *(in_hbm(leaf) for leaf in (*features, folded)))
    gathered = swap_stats(payload)
    slope, moments, payload = call(
        partial(middle_kernel, spots),
        "middle",
        (
            struct((rows - 2, PITCH, channels)),
            struct((12, channels)),
            struct((devices, 8 * parts, 128)),
        ),
        [VMEM] * 9,
        [pltpu.VMEM((8 * parts, 128), jnp.float32)],
        flops=body * channels * 100,
    )(sizes, gathered, conv_out, *cotangents, bn_gain, bn_shift)
    gathered = swap_stats(payload)
    back, send, d_gain, d_shift = call(
        partial(back_kernel, spots, devices),
        "back",
        (
            struct((cells, channels), jnp.bfloat16),
            struct((half, channels)),
            struct(bn_gain.shape),
            struct(bn_gain.shape),
        ),
        [VMEM] * 8,
        [canvas],
        flops=work // core_size,
    )(sizes, gathered, conv_out, slope, moments, bn_gain, bn_shift, spread)
    keep = call(keep_kernel, "keep", struct((half, channels)), [VMEM] * 2, flops=work // core_size)(back, spread)
    outputs = call(partial(output_kernel, spots), "output", levels, [VMEM] * 5, flops=body * channels * 100)(
        sizes, conv_out, moments, bn_gain, bn_shift
    )
    input_grads = call(
        partial(input_grad_kernel, spots),
        "input_grad",
        levels,
        [VMEM] * 3,
        [
            pltpu.VMEM((cells, 3 * channels), jnp.bfloat16),
            pltpu.VMEM((rows - 2, PITCH, channels), jnp.float32),
        ],
        flops=work,
    )(sizes, back, folded)
    parts, (outputs, input_grads) = scatter_grads(keep, send, (outputs, input_grads))
    own = call(
        partial(add_and_scale_kernel, 1.0 / devices), "add_and_scale", struct(parts[0].shape), [VMEM] * len(parts)
    )(*parts)
    weight_total = gather_grads(own).reshape(conv_weight.shape)
    return (*outputs, *input_grads, weight_total, d_gain, d_shift)


def solution(mesh):
    placed = (
        P(("wide", "group"), None, None, None),
        P(("wide", "group"), None, None, None),
        P(("wide", "group"), None, None, None),
        P(("wide", "group"), None, None, None),
        P(("wide", "group"), None, None, None),
        P(("wide", "group"), None, None, None),
        P(("wide", "group"), None, None, None),
        P(("wide", "group"), None, None, None),
        P(),
        P(),
        P(),
        P(("wide", "group")),
        P(("wide", "group")),
    )
    return jax.shard_map(
        shards,
        mesh=mesh,
        in_specs=placed,
        out_specs=(
            P(("wide", "group"), None, None, None),
            P(("wide", "group"), None, None, None),
            P(("wide", "group"), None, None, None),
            P(("wide", "group"), None, None, None),
            P(("wide", "group"), None, None, None),
            P(("wide", "group"), None, None, None),
            P(("wide", "group"), None, None, None),
            P(("wide", "group"), None, None, None),
            P(),
            P(),
            P(),
        ),
        check_vma=False,
    )
```

```python
from functools import partial

import jax
import jax.numpy as jnp
from jax import lax
from jax.experimental import pallas as pl
from jax.experimental.pallas import tpu as pltpu
from jax.sharding import PartitionSpec as P

EPSILON = 1e-05
PITCH = 32
STRIDE = 16
TURNED_CORE = 1
VMEM = pl.BlockSpec(memory_space=pltpu.VMEM)
HBM = pl.BlockSpec(memory_space=pltpu.HBM)


def canvas_spots(extents):
    spots = [(1, 0, extents[0])]
    column = 0
    for extent in extents[1:]:
        spots.append((extents[0] + 2, column, extent))
        column += -(-(extent + 1) // 8) * 8
    rows = extents[0] + extents[1] + 3
    assert column <= PITCH and extents[0] < PITCH
    return tuple(spots), rows


def level_limits(sizes_ref, level_index, extent):
    stride = STRIDE * 2**level_index
    shift = stride.bit_length() - 1
    limits = []
    for line in range(2):
        pixels = sizes_ref[line : line + 1, 0:1].reshape(1, 1, 1)
        limits.append(jnp.minimum(lax.shift_right_arithmetic(pixels + (stride - 1), shift), extent))
    return tuple(limits)


def inside_mask(limits, shape):
    row_place = lax.broadcasted_iota(jnp.int32, shape, 0)
    col_place = lax.broadcasted_iota(jnp.int32, shape, 1)
    return jnp.logical_and(row_place < limits[0], col_place < limits[1])


def put_row(ref, row, vector):
    for part in range(vector.shape[1] // 128):
        ref[row + part : row + part + 1, :] = vector[:, part * 128 : (part + 1) * 128]


def get_row(packed, level_index, parts):
    rows = [packed[level_index * parts + part : level_index * parts + part + 1, :] for part in range(parts)]
    return jnp.concatenate(rows, axis=1)


def spread_columns(flat, target):
    cells, channels = flat.shape
    target[:, 0:channels] = pltpu.roll(flat, 1, 0).astype(jnp.bfloat16)
    target[:, channels : 2 * channels] = flat.astype(jnp.bfloat16)
    target[:, 2 * channels :] = pltpu.roll(flat, cells - 1, 0).astype(jnp.bfloat16)


def forward_kernel(spots, rows, *refs):
    sizes, *features_in = refs[0:5]
    weight_in, spread_ref, conv_ref, payload_ref, canvas, packed, weight_ref, *feature_refs = refs[5:16]
    semaphores = refs[16]
    copies = [
        pltpu.make_async_copy(source, target, semaphores.at[place])
        for place, (source, target) in enumerate(
            zip(
                (*features_in, weight_in),
                (*feature_refs, weight_ref),
            )
        )
    ]
    for copy in copies:
        copy.start()
    channels = weight_ref.shape[2]
    parts = channels // 128
    canvas[...] = jnp.zeros_like(canvas)
    packed[:, 8 * channels :] = jnp.zeros((1, 128), jnp.float32)
    for copy in copies[:-1]:
        copy.wait()
    for level_index, (feat_ref, (row, column, extent)) in enumerate(zip(feature_refs, spots)):
        limits = level_limits(sizes, level_index, extent)
        values = feat_ref[0].astype(jnp.float32)
        inside = inside_mask(limits, values.shape)
        canvas[row : row + extent, column : column + extent, :] = jnp.where(inside, values, 0.0)
    spread_columns(canvas[...].reshape(rows * PITCH, channels), spread_ref)
    body = (rows - 2) * PITCH
    copies[-1].wait()
    summed = jnp.zeros((body, channels), jnp.float32)
    for tap_row in range(3):
        summed = summed + jnp.dot(
            spread_ref[tap_row * PITCH : tap_row * PITCH + body, :],
            weight_ref[tap_row],
            preferred_element_type=jnp.float32,
        )
    conv_ref[...] = summed.reshape(rows - 2, PITCH, channels)
    for level_index, (row, column, extent) in enumerate(spots):
        limits = level_limits(sizes, level_index, extent)
        conv_out = conv_ref[row - 1 : row - 1 + extent, column : column + extent, :]
        inside = inside_mask(limits, conv_out.shape)
        count = (limits[0] * limits[1]).astype(jnp.float32).reshape(1, 1)
        total = jnp.sum(jnp.where(inside, conv_out, 0.0), axis=(0, 1)).reshape(1, channels)
        centered = jnp.where(inside, conv_out - total / count, 0.0)
        spread = jnp.sum(centered * centered, axis=(0, 1)).reshape(1, channels)
        packed[:, level_index * channels : (level_index + 1) * channels] = total
        packed[:, (4 + level_index) * channels : (5 + level_index) * channels] = spread
        packed[:, 8 * channels + level_index : 8 * channels + level_index + 1] = count
    payload_ref[...] = jnp.broadcast_to(packed[...][None], payload_ref.shape)


def normalized(spots, level_index, conv_ref, moments_ref, gain_ref, bias_ref):
    row, column, extent = spots[level_index]
    mean_value = moments_ref[level_index : level_index + 1, :][None]
    inverse = moments_ref[4 + level_index : 5 + level_index, :][None]
    gain = gain_ref[level_index : level_index + 1, :][None]
    bias = bias_ref[level_index : level_index + 1, :][None]
    conv_out = conv_ref[row - 1 : row - 1 + extent, column : column + extent, :]
    normed = (conv_out - mean_value) * inverse
    return (normed, gain * normed + bias, inverse)


def middle_kernel(spots, *refs):
    sizes, gathered_ref, conv_ref, *cot_refs = refs[0:7]
    gain_ref, bias_ref, slope_ref, moments_ref, payload_ref, packed = refs[7:13]
    channels = gain_ref.shape[1]
    parts = channels // 128
    for level_index in range(4):
        sums = gathered_ref[:, :, level_index * channels : (level_index + 1) * channels]
        spreads = gathered_ref[:, :, (4 + level_index) * channels : (5 + level_index) * channels]
        counts = gathered_ref[:, :, 8 * channels + level_index : 8 * channels + level_index + 1]
        total_count = jnp.sum(counts, axis=0)
        mean_value = jnp.sum(sums, axis=0) / total_count
        offset = sums * (1.0 / counts) - mean_value[None]
        variance = jnp.sum(spreads + counts * offset * offset, axis=0) / total_count
        moments_ref[level_index : level_index + 1, :] = mean_value
        moments_ref[4 + level_index : 5 + level_index, :] = lax.rsqrt(variance + EPSILON)
        moments_ref[8 + level_index : 9 + level_index, :] = jnp.broadcast_to(total_count, (1, channels))
    for level_index, (cot_ref, (row, column, extent)) in enumerate(zip(cot_refs, spots)):
        limits = level_limits(sizes, level_index, extent)
        normed, shifted, inverse = normalized(spots, level_index, conv_ref, moments_ref, gain_ref, bias_ref)
        sigmoid_value = 1.0 / (1.0 + jnp.exp(-shifted))
        slope = cot_ref[0].astype(jnp.float32) * sigmoid_value * (1.0 + shifted * (1.0 - sigmoid_value))
        slope = jnp.where(inside_mask(limits, slope.shape), slope, 0.0)
        slope_ref[row - 1 : row - 1 + extent, column : column + extent, :] = slope
        put_row(packed, level_index * parts, jnp.sum(slope, axis=(0, 1)).reshape(1, channels))
        put_row(packed, (4 + level_index) * parts, jnp.sum(slope * normed, axis=(0, 1)).reshape(1, channels))
    payload_ref[...] = jnp.broadcast_to(packed[...][None], payload_ref.shape)


def weight_grad_rows(spread_ref, back_ref, first, target_ref):
    cells, channels = back_ref.shape
    body = cells - 2 * PITCH
    step = channels // 2
    turned = back_ref[PITCH : PITCH + body, :]
    for start in range(0, target_ref.shape[0], step):
        place = first + start
        tap_row = lax.div(place, 3 * channels)
        lane = pl.multiple_of(place - tap_row * 3 * channels, 128)
        window = spread_ref[pl.ds(pl.multiple_of(tap_row * PITCH, PITCH), body), pl.ds(lane, step)]
        target_ref[start : start + step, :] = lax.dot_general(
            window, turned, (((0,), (0,)), ((), ())), preferred_element_type=jnp.float32
        )


def back_kernel(spots, devices, *refs):
    sizes, gathered_ref, conv_ref, slope_ref, moments_ref, gain_ref, bias_ref, spread_ref = refs[0:8]
    back_ref, send_ref, d_gain_ref, d_shift_ref, wide_back = refs[8:13]
    channels = gain_ref.shape[1]
    parts = channels // 128
    block = 4 * parts
    shift_rows = jnp.sum(gathered_ref[:, 0:block, :], axis=0)
    gain_rows = jnp.sum(gathered_ref[:, block : 2 * block, :], axis=0)
    wide_back[...] = jnp.zeros_like(wide_back)
    for level_index, (row, column, extent) in enumerate(spots):
        limits = level_limits(sizes, level_index, extent)
        normed, shifted, inverse = normalized(spots, level_index, conv_ref, moments_ref, gain_ref, bias_ref)
        count = moments_ref[8 + level_index : 9 + level_index, :][None]
        shift_sum = get_row(shift_rows, level_index, parts)
        gain_sum = get_row(gain_rows, level_index, parts)
        d_gain_ref[level_index : level_index + 1, :] = gain_sum / devices
        d_shift_ref[level_index : level_index + 1, :] = shift_sum / devices
        gain = gain_ref[level_index : level_index + 1, :][None]
        slope = slope_ref[row - 1 : row - 1 + extent, column : column + extent, :]
        back = (gain * inverse) * (slope - shift_sum[None] / count - normed * (gain_sum[None] / count))
        back = jnp.where(inside_mask(limits, back.shape), back, 0.0)
        wide_back[row : row + extent, column : column + extent, :] = back
    rows = wide_back.shape[0]
    back_ref[...] = wide_back[...].reshape(rows * PITCH, channels).astype(jnp.bfloat16)
    half = send_ref.shape[0]
    core_size = (9 * channels) // half
    first = (core_size - 1 - places()[0]) * half
    weight_grad_rows(spread_ref, back_ref, first, send_ref)


def keep_kernel(back_ref, spread_ref, keep_ref):
    weight_grad_rows(spread_ref, back_ref, places()[0] * keep_ref.shape[0], keep_ref)


def output_kernel(spots, sizes, conv_ref, moments_ref, gain_ref, bias_ref, *out_refs):
    for level_index, (out_ref, (row, column, extent)) in enumerate(zip(out_refs, spots)):
        limits = level_limits(sizes, level_index, extent)
        normed, shifted, inverse = normalized(spots, level_index, conv_ref, moments_ref, gain_ref, bias_ref)
        values = shifted * (1.0 / (1.0 + jnp.exp(-shifted)))
        out_ref[0] = jnp.where(inside_mask(limits, values.shape), values, 0.0).astype(jnp.bfloat16)


def input_grad_kernel(spots, sizes, back_ref, weight_ref, *refs):
    *target_refs, spread, summed = refs
    cells, channels = back_ref.shape
    rows = cells // PITCH
    body = (rows - 2) * PITCH
    spread_columns(back_ref[...].astype(jnp.float32), spread)
    total = jnp.zeros((body, channels), jnp.float32)
    for tap_row in range(3):
        for tap_col in range(3):
            start = (2 - tap_row) * PITCH
            lane = (2 - tap_col) * channels
            total = total + lax.dot_general(
                spread[start : start + body, lane : lane + channels],
                weight_ref[tap_row, tap_col * channels : (tap_col + 1) * channels, :],
                (((1,), (1,)), ((), ())),
                preferred_element_type=jnp.float32,
            )
    summed[...] = total.reshape(rows - 2, PITCH, channels)
    for level_index, (target_ref, (row, column, extent)) in enumerate(zip(target_refs, spots)):
        limits = level_limits(sizes, level_index, extent)
        values = summed[row - 1 : row - 1 + extent, column : column + extent, :]
        target_ref[0] = jnp.where(inside_mask(limits, values.shape), values, 0.0).astype(jnp.bfloat16)


def stage_place(stage):
    return places()[stage]


def add_and_cut_kernel(stage, size, count, *refs):
    parts, pieces = refs[:count], refs[count:]
    rows = pieces[0].shape[0]
    place = stage_place(stage)
    for step, piece_ref in enumerate(pieces):
        start = pl.multiple_of(partner(place, step, size) * rows, 8)
        total = parts[0][pl.ds(start, rows), :]
        for part in parts[1:]:
            total = total + part[pl.ds(start, rows), :]
        piece_ref[...] = total


def add_and_scale_kernel(scale, *refs):
    total = refs[0][...]
    for part in refs[1:-1]:
        total = total + part[...]
    refs[-1][...] = total * scale


def join_kernel(stage, size, *refs):
    pieces, whole_ref = refs[:size], refs[size]
    rows = pieces[0].shape[0]
    place = stage_place(stage)
    for step, piece_ref in enumerate(pieces):
        start = pl.multiple_of(origin(place, step, size) * rows, 8)
        whole_ref[pl.ds(start, rows), :] = piece_ref[...]


def cut_kernel(plane_size, deep_size, count, *refs):
    parts, pieces = refs[:count], refs[count:]
    rows = pieces[1].shape[0]
    core, plane, deep = places()
    for step in range(plane_size):
        away_ref, own_ref = pieces[2 * step : 2 * step + 2]
        base = partner(plane, step, plane_size) * (rows * deep_size)
        for deep_step in range(deep_size):
            start = pl.multiple_of(base + partner(deep, deep_step, deep_size) * rows, 8)
            total = parts[0][pl.ds(start, rows), :]
            for part in parts[1:]:
                total = total + part[pl.ds(start, rows), :]
            if deep_step == 0:
                own_ref[...] = total
            else:
                away_ref[(deep_step - 1) * rows : deep_step * rows, :] = total


def add_split_kernel(count, *refs):
    parts, pieces = refs[:count], refs[count:]
    rows = pieces[0].shape[0]
    for place, piece_ref in enumerate(pieces):
        total = parts[0][place * rows : (place + 1) * rows, :]
        for part in parts[1:]:
            total = total + part[place * rows : (place + 1) * rows, :]
        piece_ref[...] = total


def lay_kernel(plane_size, core_step, *refs):
    pieces = refs[-(plane_size + 2) : -2]
    whole_ref, semaphore = refs[-2:]
    rows = pieces[0].shape[0]
    core, plane, deep = places()
    core_size, deep_size = layout()[0], layout()[3]
    if core_step and core_size == 2 and deep_size == plane_size:
        plane = deep
    first = origin(core, core_step, core_size) * (rows * plane_size)
    copies = []
    for step, piece_ref in enumerate(pieces):
        start = pl.multiple_of(first + origin(plane, step, plane_size) * rows, 8)
        target = whole_ref.at[pl.ds(start, rows), :]
        copies.append(pltpu.make_async_copy(piece_ref, target, semaphore.at[step]))
    for copy in copies:
        copy.start()
    for copy in copies:
        copy.wait()


def call(kernel, name, outputs, in_specs, scratch=(), flops=0, out_specs=None, aliases=None):
    return pl.pallas_call(
        input_output_aliases=aliases or {},
        kernel=kernel,
        out_shape=outputs,
        in_specs=in_specs,
        out_specs=jax.tree.map(lambda leaf: VMEM, outputs) if out_specs is None else out_specs,
        scratch_shapes=scratch,
        compiler_params=pltpu.CompilerParams(vmem_limit_bytes=20 * 1024 * 1024),
        cost_estimate=pl.CostEstimate(flops=flops, bytes_accessed=0, transcendentals=0),
        name=name,
    )


def layout():
    group_size = lax.axis_size("group")
    wide_size = lax.axis_size("wide")
    core_size = 2 if group_size % 2 == 0 else 1
    col_size = group_size // core_size
    row_size = col_size if wide_size % col_size == 0 else 1
    return (core_size, col_size, row_size, wide_size // row_size)


def places():
    core_size, col_size, row_size, deep_size = layout()
    group_index = lax.axis_index("group")
    wide_index = lax.axis_index("wide")
    core = lax.rem(group_index, core_size)
    plane = lax.rem(wide_index, row_size) * col_size + lax.div(group_index, core_size)
    deep = lax.div(wide_index, row_size)
    if core_size == 2 and deep_size == row_size * col_size:
        turned = core == TURNED_CORE
        plane, deep = jnp.where(turned, deep, plane), jnp.where(turned, plane, deep)
    return (core, plane, deep)


def partner(place, step, size):
    if size & (size - 1) == 0:
        return place ^ step
    return lax.rem(place + step, size) if isinstance(place, jax.Array) else (place + step) % size


def origin(place, step, size):
    return partner(place, step if size & (size - 1) == 0 else size - step, size)


def exchange(values, core_step, plane_step, deep_step):
    core_size, col_size, row_size, deep_size = layout()
    plane_size = col_size * row_size
    pairs = []
    alike = core_size == 2 and deep_size == plane_size
    for deep in range(deep_size):
        for plane in range(plane_size):
            for core in range(core_size):
                ends = []
                turn = alike and core == TURNED_CORE
                for core_end, plane_end, deep_end in (
                    (core, plane, deep),
                    (
                        partner(core, core_step, core_size),
                        partner(plane, plane_step, plane_size),
                        partner(deep, deep_step, deep_size),
                    ),
                ):
                    if turn:
                        plane_end, deep_end = deep_end, plane_end
                    wide_index = deep_end * row_size + plane_end // col_size
                    group_index = (plane_end % col_size) * core_size + core_end
                    ends.append(wide_index * col_size * core_size + group_index)
                pairs.append(tuple(ends))
    return lax.ppermute(values, ("wide", "group"), pairs)


def scatter_stage(parts, stage, size, send):
    rows, lanes = parts[0].shape
    piece_rows = rows // size
    if piece_rows % 8:
        total = sum(parts[1:], parts[0])
        pieces = [
            lax.dynamic_slice_in_dim(total, partner(places()[stage], step, size) * piece_rows, piece_rows, 0)
            for step in range(size)
        ]
    else:
        pieces = call(
            partial(add_and_cut_kernel, stage, size, len(parts)),
            "add_and_cut",
            (struct((piece_rows, lanes)),) * size,
            [VMEM] * len(parts),
            flops=rows * lanes,
        )(*parts)
    return [pieces[0]] + [send(pieces[step], step) for step in range(1, size)]


def join_stage(pieces, stage, target=None):
    rows, lanes = pieces[0].shape
    size = len(pieces)
    if rows % 8:
        whole = jnp.zeros((rows * size, lanes), pieces[0].dtype)
        for step, part in enumerate(pieces):
            start = origin(places()[stage], step, size) * rows
            whole = lax.dynamic_update_slice_in_dim(whole, part, start, 0)
        return whole
    return call(
        partial(join_kernel, stage, size),
        "join",
        struct((rows * size, lanes)),
        [VMEM] * size,
        flops=rows * size * lanes,
    )(*pieces)


def gather_stage(values, stage, size, send):
    return join_stage([values] + [send(values, step) for step in range(1, size)], stage)


def swap_stats(payload):
    return lax.all_to_all(payload, ("wide", "group"), 0, 0)


def send_core(part, step):
    return exchange(part, step, 0, 0)


def send_plane(part, step):
    return exchange(part, 0, step, 0)


def send_deep(part, step):
    return exchange(part, 0, 0, step)


def scatter_grads(keep, send):
    core_size, col_size, row_size, deep_size = layout()
    plane_size = col_size * row_size
    parts = [keep]
    if core_size > 1:
        parts.append(send_core(send, 1))
    rows, lanes = keep.shape
    rows //= plane_size * deep_size
    if rows % 8 or deep_size == 1:
        parts = scatter_stage(parts, 1, plane_size, send_plane)
        return scatter_stage(parts, 2, deep_size, send_deep)
    shapes = (struct(((deep_size - 1) * rows, lanes)), struct((rows, lanes))) * plane_size
    pieces = call(
        partial(cut_kernel, plane_size, deep_size, len(parts)), "cut", shapes, [VMEM] * len(parts), flops=keep.size
    )(*parts)
    away = [pieces[0]] + [send_plane(pieces[2 * step], step) for step in range(1, plane_size)]
    own = [pieces[1]] + [send_plane(pieces[2 * step + 1], step) for step in range(1, plane_size)]
    pieces = call(
        partial(add_split_kernel, plane_size),
        "add_split",
        (struct((rows, lanes)),) * (deep_size - 1),
        [VMEM] * plane_size,
        flops=keep.size,
    )(*away)
    return own + [send_deep(piece, step + 1) for step, piece in enumerate(pieces)]


def gather_grads(own, beside):
    core_size, col_size, row_size, deep_size = layout()
    plane_size = col_size * row_size
    rows, lanes = own.shape
    half = rows * plane_size * deep_size
    if rows % 8 or deep_size == 1:
        own = gather_stage(own, 2, deep_size, send_deep)
        own = gather_stage(own, 1, plane_size, send_plane)
        return (gather_stage(own, 0, core_size, send_core), beside)
    own = gather_stage(own, 2, deep_size, send_deep)
    pieces = [own] + [send_plane(own, step) for step in range(1, plane_size)]
    if plane_size > 1:
        pieces[-1], beside = lax.optimization_barrier((pieces[-1], beside))
    shape = struct((half * core_size, lanes))
    scratch = [pltpu.SemaphoreType.DMA((plane_size,))]
    total = call(
        partial(lay_kernel, plane_size, 0), "lay", shape, [VMEM] * plane_size, scratch, half * lanes, HBM
    )(*pieces)
    for core_step in range(1, core_size):
        others = [send_core(piece, core_step) for piece in pieces]
        total = call(
            partial(lay_kernel, plane_size, core_step),
            "lay_other",
            shape,
            [HBM] + [VMEM] * plane_size,
            scratch,
            half * lanes,
            HBM,
            {0: 0},
        )(total, *others)
    return (total, beside)


def in_hbm(leaf):
    return pltpu.with_memory_space_constraint(leaf, pltpu.HBM)


def struct(shape, dtype=jnp.float32):
    return jax.ShapeDtypeStruct(shape, dtype)


def shards(
    feat4,
    feat5,
    feat6,
    feat7,
    out_grad4,
    out_grad5,
    out_grad6,
    out_grad7,
    conv_weight,
    bn_gain,
    bn_shift,
    heights,
    widths,
):
    features = (feat4, feat5, feat6, feat7)
    cotangents = (out_grad4, out_grad5, out_grad6, out_grad7)
    devices = lax.axis_size("wide") * lax.axis_size("group")
    core_size = layout()[0]
    channels = conv_weight.shape[2]
    parts = channels // 128
    spots, rows = canvas_spots(tuple(feature.shape[1] for feature in features))
    cells = rows * PITCH
    body = cells - 2 * PITCH
    folded = conv_weight.reshape(3, 3 * channels, channels)
    work = 2 * body * 9 * channels * channels
    half = 9 * channels // core_size
    levels = tuple(struct(feature.shape, jnp.bfloat16) for feature in features)
    canvas = pltpu.VMEM((rows, PITCH, channels), jnp.float32)

    sizes = jnp.concatenate([heights, widths]).reshape(2, 1)
    spread, conv_out, payload = call(
        partial(forward_kernel, spots, rows),
        "forward",
        (
            struct((cells, 3 * channels), jnp.bfloat16),
            struct((rows - 2, PITCH, channels)),
            struct((devices, 1, 8 * channels + 128)),
        ),
        [VMEM] + [HBM] * 5,
        [canvas, pltpu.VMEM((1, 8 * channels + 128), jnp.float32), pltpu.VMEM(folded.shape, folded.dtype)]
        + [pltpu.VMEM(feature.shape, feature.dtype) for feature in features]
        + [pltpu.SemaphoreType.DMA((5,))],
        flops=work,
    )(sizes, *(in_hbm(leaf) for leaf in (*features, folded)))
    gathered = swap_stats(payload)
    slope, moments, payload = call(
        partial(middle_kernel, spots),
        "middle",
        (
            struct((rows - 2, PITCH, channels)),
            struct((12, channels)),
            struct((devices, 8 * parts, 128)),
        ),
        [VMEM] * 9,
        [pltpu.VMEM((8 * parts, 128), jnp.float32)],
        flops=body * channels * 100,
    )(sizes, gathered, conv_out, *cotangents, bn_gain, bn_shift)
    gathered = swap_stats(payload)
    back, send, d_gain, d_shift = call(
        partial(back_kernel, spots, devices),
        "back",
        (
            struct((cells, channels), jnp.bfloat16),
            struct((half, channels)),
            struct(bn_gain.shape),
            struct(bn_gain.shape),
        ),
        [VMEM] * 8,
        [canvas],
        flops=work // core_size,
    )(sizes, gathered, conv_out, slope, moments, bn_gain, bn_shift, spread)
    keep = call(keep_kernel, "keep", struct((half, channels)), [VMEM] * 2, flops=work // core_size)(back, spread)
    outputs = call(partial(output_kernel, spots), "output", levels, [VMEM] * 5, flops=body * channels * 100)(
        sizes, conv_out, moments, bn_gain, bn_shift
    )
    input_grads = call(
        partial(input_grad_kernel, spots),
        "input_grad",
        levels,
        [VMEM] * 3,
        [
            pltpu.VMEM((cells, 3 * channels), jnp.bfloat16),
            pltpu.VMEM((rows - 2, PITCH, channels), jnp.float32),
        ],
        flops=work,
    )(sizes, back, folded)
    parts = scatter_grads(keep, send)
    own = call(
        partial(add_and_scale_kernel, 1.0 / devices), "add_and_scale", struct(parts[0].shape), [VMEM] * len(parts)
    )(*parts)
    weight_total, (outputs, input_grads) = gather_grads(own, (outputs, input_grads))
    weight_total = weight_total.reshape(conv_weight.shape)
    return (*outputs, *input_grads, weight_total, d_gain, d_shift)


def solution(mesh):
    placed = (
        P(("wide", "group"), None, None, None),
        P(("wide", "group"), None, None, None),
        P(("wide", "group"), None, None, None),
        P(("wide", "group"), None, None, None),
        P(("wide", "group"), None, None, None),
        P(("wide", "group"), None, None, None),
        P(("wide", "group"), None, None, None),
        P(("wide", "group"), None, None, None),
        P(),
        P(),
        P(),
        P(("wide", "group")),
        P(("wide", "group")),
    )
    return jax.shard_map(
        shards,
        mesh=mesh,
        in_specs=placed,
        out_specs=(
            P(("wide", "group"), None, None, None),
            P(("wide", "group"), None, None, None),
            P(("wide", "group"), None, None, None),
            P(("wide", "group"), None, None, None),
            P(("wide", "group"), None, None, None),
            P(("wide", "group"), None, None, None),
            P(("wide", "group"), None, None, None),
            P(("wide", "group"), None, None, None),
            P(),
            P(),
            P(),
        ),
        check_vma=False,
    )
```

```python
from functools import partial

import jax
import jax.numpy as jnp
from jax import lax
from jax.experimental import pallas as pl
from jax.experimental.pallas import tpu as pltpu
from jax.sharding import PartitionSpec as P

EPSILON = 1e-05
PITCH = 32
STRIDE = 16
TURNED_CORE = 1
VMEM = pl.BlockSpec(memory_space=pltpu.VMEM)
HBM = pl.BlockSpec(memory_space=pltpu.HBM)


def canvas_spots(extents):
    spots = [(1, 0, extents[0])]
    column = 0
    for extent in extents[1:]:
        spots.append((extents[0] + 2, column, extent))
        column += -(-(extent + 1) // 8) * 8
    rows = extents[0] + extents[1] + 3
    assert column <= PITCH and extents[0] < PITCH
    return tuple(spots), rows


def level_limits(sizes_ref, level_index, extent):
    stride = STRIDE * 2**level_index
    shift = stride.bit_length() - 1
    limits = []
    for line in range(2):
        pixels = sizes_ref[line : line + 1, 0:1].reshape(1, 1, 1)
        limits.append(jnp.minimum(lax.shift_right_arithmetic(pixels + (stride - 1), shift), extent))
    return tuple(limits)


def inside_mask(limits, shape):
    row_place = lax.broadcasted_iota(jnp.int32, shape, 0)
    col_place = lax.broadcasted_iota(jnp.int32, shape, 1)
    return jnp.logical_and(row_place < limits[0], col_place < limits[1])


def put_row(ref, row, vector):
    for part in range(vector.shape[1] // 128):
        ref[row + part : row + part + 1, :] = vector[:, part * 128 : (part + 1) * 128]


def get_row(packed, level_index, parts):
    rows = [packed[level_index * parts + part : level_index * parts + part + 1, :] for part in range(parts)]
    return jnp.concatenate(rows, axis=1)


def spread_columns(flat, target):
    cells, channels = flat.shape
    target[:, 0:channels] = pltpu.roll(flat, 1, 0).astype(jnp.bfloat16)
    target[:, channels : 2 * channels] = flat.astype(jnp.bfloat16)
    target[:, 2 * channels :] = pltpu.roll(flat, cells - 1, 0).astype(jnp.bfloat16)


def forward_kernel(spots, rows, *refs):
    sizes, *features_in = refs[0:5]
    weight_in, spread_ref, conv_ref, payload_ref, canvas, packed, weight_ref, *feature_refs = refs[5:16]
    semaphores = refs[16]
    copies = [
        pltpu.make_async_copy(source, target, semaphores.at[place])
        for place, (source, target) in enumerate(
            zip(
                (*features_in, weight_in),
                (*feature_refs, weight_ref),
            )
        )
    ]
    for copy in copies:
        copy.start()
    channels = weight_ref.shape[2]
    parts = channels // 128
    canvas[...] = jnp.zeros_like(canvas)
    packed[:, 8 * channels :] = jnp.zeros((1, 128), jnp.float32)
    for copy in copies[:-1]:
        copy.wait()
    for level_index, (feat_ref, (row, column, extent)) in enumerate(zip(feature_refs, spots)):
        limits = level_limits(sizes, level_index, extent)
        values = feat_ref[0].astype(jnp.float32)
        inside = inside_mask(limits, values.shape)
        canvas[row : row + extent, column : column + extent, :] = jnp.where(inside, values, 0.0)
    spread_columns(canvas[...].reshape(rows * PITCH, channels), spread_ref)
    copies[-1].wait()
    for first in range(0, rows - 2, 8):
        lines = min(8, rows - 2 - first)
        summed = jnp.zeros((lines * PITCH, channels), jnp.float32)
        for tap_row in range(3):
            start = (first + tap_row) * PITCH
            summed = summed + jnp.dot(
                spread_ref[start : start + lines * PITCH, :], weight_ref[tap_row], preferred_element_type=jnp.float32
            )
        conv_ref[first : first + lines] = summed.reshape(lines, PITCH, channels)
    for level_index, (row, column, extent) in enumerate(spots):
        limits = level_limits(sizes, level_index, extent)
        conv_out = conv_ref[row - 1 : row - 1 + extent, column : column + extent, :]
        inside = inside_mask(limits, conv_out.shape)
        count = (limits[0] * limits[1]).astype(jnp.float32).reshape(1, 1)
        total = jnp.sum(jnp.where(inside, conv_out, 0.0), axis=(0, 1)).reshape(1, channels)
        centered = jnp.where(inside, conv_out - total / count, 0.0)
        spread = jnp.sum(centered * centered, axis=(0, 1)).reshape(1, channels)
        packed[:, level_index * channels : (level_index + 1) * channels] = total
        packed[:, (4 + level_index) * channels : (5 + level_index) * channels] = spread
        packed[:, 8 * channels + level_index : 8 * channels + level_index + 1] = count
    payload_ref[...] = jnp.broadcast_to(packed[...][None], payload_ref.shape)


def normalized(spots, level_index, conv_ref, moments_ref, gain_ref, bias_ref):
    row, column, extent = spots[level_index]
    mean_value = moments_ref[level_index : level_index + 1, :][None]
    inverse = moments_ref[4 + level_index : 5 + level_index, :][None]
    gain = gain_ref[level_index : level_index + 1, :][None]
    bias = bias_ref[level_index : level_index + 1, :][None]
    conv_out = conv_ref[row - 1 : row - 1 + extent, column : column + extent, :]
    normed = (conv_out - mean_value) * inverse
    return (normed, gain * normed + bias, inverse)


def middle_kernel(spots, *refs):
    sizes, gathered_ref, conv_ref, *cot_refs = refs[0:7]
    gain_ref, bias_ref, slope_ref, moments_ref, payload_ref, packed = refs[7:13]
    channels = gain_ref.shape[1]
    parts = channels // 128
    for level_index in range(4):
        sums = gathered_ref[:, :, level_index * channels : (level_index + 1) * channels]
        spreads = gathered_ref[:, :, (4 + level_index) * channels : (5 + level_index) * channels]
        counts = gathered_ref[:, :, 8 * channels + level_index : 8 * channels + level_index + 1]
        total_count = jnp.sum(counts, axis=0)
        mean_value = jnp.sum(sums, axis=0) / total_count
        offset = sums * (1.0 / counts) - mean_value[None]
        variance = jnp.sum(spreads + counts * offset * offset, axis=0) / total_count
        moments_ref[level_index : level_index + 1, :] = mean_value
        moments_ref[4 + level_index : 5 + level_index, :] = lax.rsqrt(variance + EPSILON)
        moments_ref[8 + level_index : 9 + level_index, :] = jnp.broadcast_to(total_count, (1, channels))
    for level_index, (cot_ref, (row, column, extent)) in enumerate(zip(cot_refs, spots)):
        limits = level_limits(sizes, level_index, extent)
        normed, shifted, inverse = normalized(spots, level_index, conv_ref, moments_ref, gain_ref, bias_ref)
        sigmoid_value = 1.0 / (1.0 + jnp.exp(-shifted))
        slope = cot_ref[0].astype(jnp.float32) * sigmoid_value * (1.0 + shifted * (1.0 - sigmoid_value))
        slope = jnp.where(inside_mask(limits, slope.shape), slope, 0.0)
        slope_ref[row - 1 : row - 1 + extent, column : column + extent, :] = slope
        put_row(packed, level_index * parts, jnp.sum(slope, axis=(0, 1)).reshape(1, channels))
        put_row(packed, (4 + level_index) * parts, jnp.sum(slope * normed, axis=(0, 1)).reshape(1, channels))
    payload_ref[...] = jnp.broadcast_to(packed[...][None], payload_ref.shape)


def weight_grad_rows(spread_ref, back_ref, first, target_ref):
    cells, channels = back_ref.shape
    body = cells - 2 * PITCH
    step = channels // 2
    turned = back_ref[PITCH : PITCH + body, :]
    for start in range(0, target_ref.shape[0], step):
        place = first + start
        tap_row = lax.div(place, 3 * channels)
        lane = pl.multiple_of(place - tap_row * 3 * channels, 128)
        window = spread_ref[pl.ds(pl.multiple_of(tap_row * PITCH, PITCH), body), pl.ds(lane, step)]
        target_ref[start : start + step, :] = lax.dot_general(
            window, turned, (((0,), (0,)), ((), ())), preferred_element_type=jnp.float32
        )


def back_kernel(spots, devices, *refs):
    sizes, gathered_ref, conv_ref, slope_ref, moments_ref, gain_ref, bias_ref, spread_ref = refs[0:8]
    back_ref, send_ref, d_gain_ref, d_shift_ref, wide_back = refs[8:13]
    channels = gain_ref.shape[1]
    parts = channels // 128
    block = 4 * parts
    shift_rows = jnp.sum(gathered_ref[:, 0:block, :], axis=0)
    gain_rows = jnp.sum(gathered_ref[:, block : 2 * block, :], axis=0)
    wide_back[...] = jnp.zeros_like(wide_back)
    for level_index, (row, column, extent) in enumerate(spots):
        limits = level_limits(sizes, level_index, extent)
        normed, shifted, inverse = normalized(spots, level_index, conv_ref, moments_ref, gain_ref, bias_ref)
        count = moments_ref[8 + level_index : 9 + level_index, :][None]
        shift_sum = get_row(shift_rows, level_index, parts)
        gain_sum = get_row(gain_rows, level_index, parts)
        d_gain_ref[level_index : level_index + 1, :] = gain_sum / devices
        d_shift_ref[level_index : level_index + 1, :] = shift_sum / devices
        gain = gain_ref[level_index : level_index + 1, :][None]
        slope = slope_ref[row - 1 : row - 1 + extent, column : column + extent, :]
        back = (gain * inverse) * (slope - shift_sum[None] / count - normed * (gain_sum[None] / count))
        back = jnp.where(inside_mask(limits, back.shape), back, 0.0)
        wide_back[row : row + extent, column : column + extent, :] = back
    rows = wide_back.shape[0]
    back_ref[...] = wide_back[...].reshape(rows * PITCH, channels).astype(jnp.bfloat16)
    half = send_ref.shape[0]
    core_size = (9 * channels) // half
    first = (core_size - 1 - places()[0]) * half
    weight_grad_rows(spread_ref, back_ref, first, send_ref)


def keep_kernel(back_ref, spread_ref, keep_ref):
    weight_grad_rows(spread_ref, back_ref, places()[0] * keep_ref.shape[0], keep_ref)


def output_kernel(spots, sizes, conv_ref, moments_ref, gain_ref, bias_ref, *out_refs):
    for level_index, (out_ref, (row, column, extent)) in enumerate(zip(out_refs, spots)):
        limits = level_limits(sizes, level_index, extent)
        normed, shifted, inverse = normalized(spots, level_index, conv_ref, moments_ref, gain_ref, bias_ref)
        values = shifted * (1.0 / (1.0 + jnp.exp(-shifted)))
        out_ref[0] = jnp.where(inside_mask(limits, values.shape), values, 0.0).astype(jnp.bfloat16)


def input_grad_kernel(spots, sizes, back_ref, weight_ref, *refs):
    *target_refs, spread, summed = refs
    cells, channels = back_ref.shape
    rows = cells // PITCH
    body = (rows - 2) * PITCH
    spread_columns(back_ref[...].astype(jnp.float32), spread)
    total = jnp.zeros((body, channels), jnp.float32)
    for tap_row in range(3):
        for tap_col in range(3):
            start = (2 - tap_row) * PITCH
            lane = (2 - tap_col) * channels
            total = total + lax.dot_general(
                spread[start : start + body, lane : lane + channels],
                weight_ref[tap_row, tap_col * channels : (tap_col + 1) * channels, :],
                (((1,), (1,)), ((), ())),
                preferred_element_type=jnp.float32,
            )
    summed[...] = total.reshape(rows - 2, PITCH, channels)
    for level_index, (target_ref, (row, column, extent)) in enumerate(zip(target_refs, spots)):
        limits = level_limits(sizes, level_index, extent)
        values = summed[row - 1 : row - 1 + extent, column : column + extent, :]
        target_ref[0] = jnp.where(inside_mask(limits, values.shape), values, 0.0).astype(jnp.bfloat16)


def stage_place(stage):
    return places()[stage]


def add_and_cut_kernel(stage, size, count, *refs):
    parts, pieces = refs[:count], refs[count:]
    rows = pieces[0].shape[0]
    place = stage_place(stage)
    for step, piece_ref in enumerate(pieces):
        start = pl.multiple_of(partner(place, step, size) * rows, 8)
        total = parts[0][pl.ds(start, rows), :]
        for part in parts[1:]:
            total = total + part[pl.ds(start, rows), :]
        piece_ref[...] = total


def add_and_scale_kernel(scale, *refs):
    total = refs[0][...]
    for part in refs[1:-1]:
        total = total + part[...]
    refs[-1][...] = total * scale


def join_kernel(stage, size, *refs):
    pieces, whole_ref = refs[:size], refs[size]
    rows = pieces[0].shape[0]
    place = stage_place(stage)
    for step, piece_ref in enumerate(pieces):
        start = pl.multiple_of(origin(place, step, size) * rows, 8)
        whole_ref[pl.ds(start, rows), :] = piece_ref[...]


def cut_kernel(plane_size, deep_size, count, *refs):
    parts, pieces = refs[:count], refs[count:]
    rows = pieces[1].shape[0]
    core, plane, deep = places()
    for step in range(plane_size):
        away_ref, own_ref = pieces[2 * step : 2 * step + 2]
        base = partner(plane, step, plane_size) * (rows * deep_size)
        for deep_step in range(deep_size):
            start = pl.multiple_of(base + partner(deep, deep_step, deep_size) * rows, 8)
            total = parts[0][pl.ds(start, rows), :]
            for part in parts[1:]:
                total = total + part[pl.ds(start, rows), :]
            if deep_step == 0:
                own_ref[...] = total
            else:
                away_ref[(deep_step - 1) * rows : deep_step * rows, :] = total


def add_split_kernel(count, *refs):
    parts, pieces = refs[:count], refs[count:]
    rows = pieces[0].shape[0]
    for place, piece_ref in enumerate(pieces):
        total = parts[0][place * rows : (place + 1) * rows, :]
        for part in parts[1:]:
            total = total + part[place * rows : (place + 1) * rows, :]
        piece_ref[...] = total


def lay_kernel(plane_size, core_step, *refs):
    pieces = refs[-(plane_size + 2) : -2]
    whole_ref, semaphore = refs[-2:]
    rows = pieces[0].shape[0]
    core, plane, deep = places()
    core_size, deep_size = layout()[0], layout()[3]
    if core_step and core_size == 2 and deep_size == plane_size:
        plane = deep
    first = origin(core, core_step, core_size) * (rows * plane_size)
    copies = []
    for step, piece_ref in enumerate(pieces):
        start = pl.multiple_of(first + origin(plane, step, plane_size) * rows, 8)
        target = whole_ref.at[pl.ds(start, rows), :]
        copies.append(pltpu.make_async_copy(piece_ref, target, semaphore.at[step]))
    for copy in copies:
        copy.start()
    for copy in copies:
        copy.wait()


def call(kernel, name, outputs, in_specs, scratch=(), flops=0, out_specs=None, aliases=None):
    return pl.pallas_call(
        input_output_aliases=aliases or {},
        kernel=kernel,
        out_shape=outputs,
        in_specs=in_specs,
        out_specs=jax.tree.map(lambda leaf: VMEM, outputs) if out_specs is None else out_specs,
        scratch_shapes=scratch,
        compiler_params=pltpu.CompilerParams(vmem_limit_bytes=20 * 1024 * 1024),
        cost_estimate=pl.CostEstimate(flops=flops, bytes_accessed=0, transcendentals=0),
        name=name,
    )


def layout():
    group_size = lax.axis_size("group")
    wide_size = lax.axis_size("wide")
    core_size = 2 if group_size % 2 == 0 else 1
    col_size = group_size // core_size
    row_size = col_size if wide_size % col_size == 0 else 1
    return (core_size, col_size, row_size, wide_size // row_size)


def places():
    core_size, col_size, row_size, deep_size = layout()
    group_index = lax.axis_index("group")
    wide_index = lax.axis_index("wide")
    core = lax.rem(group_index, core_size)
    plane = lax.rem(wide_index, row_size) * col_size + lax.div(group_index, core_size)
    deep = lax.div(wide_index, row_size)
    if core_size == 2 and deep_size == row_size * col_size:
        turned = core == TURNED_CORE
        plane, deep = jnp.where(turned, deep, plane), jnp.where(turned, plane, deep)
    return (core, plane, deep)


def partner(place, step, size):
    if size & (size - 1) == 0:
        return place ^ step
    return lax.rem(place + step, size) if isinstance(place, jax.Array) else (place + step) % size


def origin(place, step, size):
    return partner(place, step if size & (size - 1) == 0 else size - step, size)


def exchange(values, core_step, plane_step, deep_step):
    core_size, col_size, row_size, deep_size = layout()
    plane_size = col_size * row_size
    pairs = []
    alike = core_size == 2 and deep_size == plane_size
    for deep in range(deep_size):
        for plane in range(plane_size):
            for core in range(core_size):
                ends = []
                turn = alike and core == TURNED_CORE
                for core_end, plane_end, deep_end in (
                    (core, plane, deep),
                    (
                        partner(core, core_step, core_size),
                        partner(plane, plane_step, plane_size),
                        partner(deep, deep_step, deep_size),
                    ),
                ):
                    if turn:
                        plane_end, deep_end = deep_end, plane_end
                    wide_index = deep_end * row_size + plane_end // col_size
                    group_index = (plane_end % col_size) * core_size + core_end
                    ends.append(wide_index * col_size * core_size + group_index)
                pairs.append(tuple(ends))
    return lax.ppermute(values, ("wide", "group"), pairs)


def scatter_stage(parts, stage, size, send):
    rows, lanes = parts[0].shape
    piece_rows = rows // size
    if piece_rows % 8:
        total = sum(parts[1:], parts[0])
        pieces = [
            lax.dynamic_slice_in_dim(total, partner(places()[stage], step, size) * piece_rows, piece_rows, 0)
            for step in range(size)
        ]
    else:
        pieces = call(
            partial(add_and_cut_kernel, stage, size, len(parts)),
            "add_and_cut",
            (struct((piece_rows, lanes)),) * size,
            [VMEM] * len(parts),
            flops=rows * lanes,
        )(*parts)
    return [pieces[0]] + [send(pieces[step], step) for step in range(1, size)]


def join_stage(pieces, stage, target=None):
    rows, lanes = pieces[0].shape
    size = len(pieces)
    if rows % 8:
        whole = jnp.zeros((rows * size, lanes), pieces[0].dtype)
        for step, part in enumerate(pieces):
            start = origin(places()[stage], step, size) * rows
            whole = lax.dynamic_update_slice_in_dim(whole, part, start, 0)
        return whole
    return call(
        partial(join_kernel, stage, size),
        "join",
        struct((rows * size, lanes)),
        [VMEM] * size,
        flops=rows * size * lanes,
    )(*pieces)


def gather_stage(values, stage, size, send):
    return join_stage([values] + [send(values, step) for step in range(1, size)], stage)


def swap_stats(payload):
    return lax.all_to_all(payload, ("wide", "group"), 0, 0)


def send_core(part, step):
    return exchange(part, step, 0, 0)


def send_plane(part, step):
    return exchange(part, 0, step, 0)


def send_deep(part, step):
    return exchange(part, 0, 0, step)


def scatter_grads(keep, send):
    core_size, col_size, row_size, deep_size = layout()
    plane_size = col_size * row_size
    parts = [keep]
    if core_size > 1:
        parts.append(send_core(send, 1))
    rows, lanes = keep.shape
    rows //= plane_size * deep_size
    if rows % 8 or deep_size == 1:
        parts = scatter_stage(parts, 1, plane_size, send_plane)
        return scatter_stage(parts, 2, deep_size, send_deep)
    shapes = (struct(((deep_size - 1) * rows, lanes)), struct((rows, lanes))) * plane_size
    pieces = call(
        partial(cut_kernel, plane_size, deep_size, len(parts)), "cut", shapes, [VMEM] * len(parts), flops=keep.size
    )(*parts)
    away = [pieces[0]] + [send_plane(pieces[2 * step], step) for step in range(1, plane_size)]
    own = [pieces[1]] + [send_plane(pieces[2 * step + 1], step) for step in range(1, plane_size)]
    pieces = call(
        partial(add_split_kernel, plane_size),
        "add_split",
        (struct((rows, lanes)),) * (deep_size - 1),
        [VMEM] * plane_size,
        flops=keep.size,
    )(*away)
    return own + [send_deep(piece, step + 1) for step, piece in enumerate(pieces)]


def gather_grads(own, beside):
    core_size, col_size, row_size, deep_size = layout()
    plane_size = col_size * row_size
    rows, lanes = own.shape
    half = rows * plane_size * deep_size
    if rows % 8 or deep_size == 1:
        own = gather_stage(own, 2, deep_size, send_deep)
        own = gather_stage(own, 1, plane_size, send_plane)
        return (gather_stage(own, 0, core_size, send_core), beside)
    own = gather_stage(own, 2, deep_size, send_deep)
    pieces = [own] + [send_plane(own, step) for step in range(1, plane_size)]
    if plane_size > 1:
        pieces[-1], beside = lax.optimization_barrier((pieces[-1], beside))
    shape = struct((half * core_size, lanes))
    scratch = [pltpu.SemaphoreType.DMA((plane_size,))]
    total = call(
        partial(lay_kernel, plane_size, 0), "lay", shape, [VMEM] * plane_size, scratch, half * lanes, HBM
    )(*pieces)
    for core_step in range(1, core_size):
        others = [send_core(piece, core_step) for piece in pieces]
        total = call(
            partial(lay_kernel, plane_size, core_step),
            "lay_other",
            shape,
            [HBM] + [VMEM] * plane_size,
            scratch,
            half * lanes,
            HBM,
            {0: 0},
        )(total, *others)
    return (total, beside)


def in_hbm(leaf):
    return pltpu.with_memory_space_constraint(leaf, pltpu.HBM)


def struct(shape, dtype=jnp.float32):
    return jax.ShapeDtypeStruct(shape, dtype)


def shards(
    feat4,
    feat5,
    feat6,
    feat7,
    out_grad4,
    out_grad5,
    out_grad6,
    out_grad7,
    conv_weight,
    bn_gain,
    bn_shift,
    heights,
    widths,
):
    features = (feat4, feat5, feat6, feat7)
    cotangents = (out_grad4, out_grad5, out_grad6, out_grad7)
    devices = lax.axis_size("wide") * lax.axis_size("group")
    core_size = layout()[0]
    channels = conv_weight.shape[2]
    parts = channels // 128
    spots, rows = canvas_spots(tuple(feature.shape[1] for feature in features))
    cells = rows * PITCH
    body = cells - 2 * PITCH
    folded = conv_weight.reshape(3, 3 * channels, channels)
    work = 2 * body * 9 * channels * channels
    half = 9 * channels // core_size
    levels = tuple(struct(feature.shape, jnp.bfloat16) for feature in features)
    canvas = pltpu.VMEM((rows, PITCH, channels), jnp.float32)

    sizes = jnp.concatenate([heights, widths]).reshape(2, 1)
    spread, conv_out, payload = call(
        partial(forward_kernel, spots, rows),
        "forward",
        (
            struct((cells, 3 * channels), jnp.bfloat16),
            struct((rows - 2, PITCH, channels)),
            struct((devices, 1, 8 * channels + 128)),
        ),
        [VMEM] + [HBM] * 5,
        [canvas, pltpu.VMEM((1, 8 * channels + 128), jnp.float32), pltpu.VMEM(folded.shape, folded.dtype)]
        + [pltpu.VMEM(feature.shape, feature.dtype) for feature in features]
        + [pltpu.SemaphoreType.DMA((5,))],
        flops=work,
    )(sizes, *(in_hbm(leaf) for leaf in (*features, folded)))
    gathered = swap_stats(payload)
    slope, moments, payload = call(
        partial(middle_kernel, spots),
        "middle",
        (
            struct((rows - 2, PITCH, channels)),
            struct((12, channels)),
            struct((devices, 8 * parts, 128)),
        ),
        [VMEM] * 9,
        [pltpu.VMEM((8 * parts, 128), jnp.float32)],
        flops=body * channels * 100,
    )(sizes, gathered, conv_out, *cotangents, bn_gain, bn_shift)
    gathered = swap_stats(payload)
    back, send, d_gain, d_shift = call(
        partial(back_kernel, spots, devices),
        "back",
        (
            struct((cells, channels), jnp.bfloat16),
            struct((half, channels)),
            struct(bn_gain.shape),
            struct(bn_gain.shape),
        ),
        [VMEM] * 8,
        [canvas],
        flops=work // core_size,
    )(sizes, gathered, conv_out, slope, moments, bn_gain, bn_shift, spread)
    keep = call(keep_kernel, "keep", struct((half, channels)), [VMEM] * 2, flops=work // core_size)(back, spread)
    outputs = call(partial(output_kernel, spots), "output", levels, [VMEM] * 5, flops=body * channels * 100)(
        sizes, conv_out, moments, bn_gain, bn_shift
    )
    input_grads = call(
        partial(input_grad_kernel, spots),
        "input_grad",
        levels,
        [VMEM] * 3,
        [
            pltpu.VMEM((cells, 3 * channels), jnp.bfloat16),
            pltpu.VMEM((rows - 2, PITCH, channels), jnp.float32),
        ],
        flops=work,
    )(sizes, back, folded)
    parts = scatter_grads(keep, send)
    own = call(
        partial(add_and_scale_kernel, 1.0 / devices), "add_and_scale", struct(parts[0].shape), [VMEM] * len(parts)
    )(*parts)
    weight_total, (outputs, input_grads) = gather_grads(own, (outputs, input_grads))
    weight_total = weight_total.reshape(conv_weight.shape)
    return (*outputs, *input_grads, weight_total, d_gain, d_shift)


def solution(mesh):
    placed = (
        P(("wide", "group"), None, None, None),
        P(("wide", "group"), None, None, None),
        P(("wide", "group"), None, None, None),
        P(("wide", "group"), None, None, None),
        P(("wide", "group"), None, None, None),
        P(("wide", "group"), None, None, None),
        P(("wide", "group"), None, None, None),
        P(("wide", "group"), None, None, None),
        P(),
        P(),
        P(),
        P(("wide", "group")),
        P(("wide", "group")),
    )
    return jax.shard_map(
        shards,
        mesh=mesh,
        in_specs=placed,
        out_specs=(
            P(("wide", "group"), None, None, None),
            P(("wide", "group"), None, None, None),
            P(("wide", "group"), None, None, None),
            P(("wide", "group"), None, None, None),
            P(("wide", "group"), None, None, None),
            P(("wide", "group"), None, None, None),
            P(("wide", "group"), None, None, None),
            P(("wide", "group"), None, None, None),
            P(),
            P(),
            P(),
        ),
        check_vma=False,
    )
```
